32 devices in a mesh: rep: 4 (over z), rows: 8 (over y, x, core).
Axes of the slice: x: 2, y: 2, z: 4, core: 2. Of those that a mesh axis runs over, the one named last changes fastest.
Arguments:
- adjacency: bfloat16 [24576, 24576], P('rows', 'rep')
- block_mask: int32 [8, 8], replicated
- features: bfloat16 [24576, 100], P('rows')
- w_one: bfloat16 [100, 256], replicated
- w_two: bfloat16 [256, 47], replicated
Outputs:
- output: float32 [24576, 47], P('rows')
All inputs are finite; a program needn't handle non-finite values.
Results may differ from the reference program's by a relative error of at most 0.001.
Values are sent between devices in bfloat16 or wider.
A program may use at most 1 GiB of HBM per device.

```python
import jax
import jax.numpy as jnp
from jax import lax

ROWS = 8
BLOCK = 3072
F0 = 100
F1 = 256
F2 = 47

NODES = ROWS * BLOCK


def draw_mask(key):
    key_w, key_r = jax.random.split(key)
    weight = jax.random.randint(key_w, (ROWS,), 1, 5, dtype=jnp.int32)
    pair_draws = jnp.triu(jax.random.randint(key_r, (ROWS, ROWS), 0, 10, dtype=jnp.int32), 1)
    pair_draws = pair_draws + pair_draws.T
    block_ids = jnp.arange(ROWS)
    diag_pair = block_ids[:, None] == block_ids[None, :]
    keep_pair = pair_draws < weight[:, None] + weight[None, :]
    return (keep_pair | diag_pair).astype(jnp.int32)


def hash_rows(row_x, row_y, node_x, node_y):
    hash_bits = row_x[:, None] * node_x[None, :] + (row_y[:, None] ^ node_y[None, :])
    hash_bits = hash_bits ^ (hash_bits >> 15)
    hash_bits = hash_bits * 73244475
    return hash_bits ^ (hash_bits >> 13)


def build_adjacency(key, block_mask):
    key_x, key_y = jax.random.split(key)
    node_x = jax.random.randint(key_x, (NODES,), 0, 2 ** 30, dtype=jnp.int32)
    node_y = jax.random.randint(key_y, (NODES,), 0, 2 ** 30, dtype=jnp.int32)
    col_ids = jnp.arange(NODES)

    def edge_rows(blk_idx):
        row_start = blk_idx * BLOCK
        row_ids = row_start + jnp.arange(BLOCK)
        hash_bits = hash_rows(lax.dynamic_slice_in_dim(node_x, row_start, BLOCK), lax.dynamic_slice_in_dim(node_y, row_start, BLOCK), node_x, node_y)
        col_keep = jnp.repeat(block_mask[blk_idx], BLOCK) == 1
        self_loop = row_ids[:, None] == col_ids[None, :]
        linked = ((hash_bits & 7) == 0) & col_keep[None, :] & jnp.logical_not(self_loop)
        return (linked | self_loop).astype(jnp.float32)

    degree = lax.map(lambda blk_idx: jnp.sum(edge_rows(blk_idx), axis=1), jnp.arange(ROWS)).reshape(NODES)
    inv_root = lax.rsqrt(degree)

    def scaled_rows(blk_idx):
        row_scale = lax.dynamic_slice_in_dim(inv_root, blk_idx * BLOCK, BLOCK)
        return (edge_rows(blk_idx) * row_scale[:, None] * inv_root[None, :]).astype(jnp.bfloat16)

    adjacency = lax.map(scaled_rows, jnp.arange(ROWS)).reshape(NODES, NODES)
    return adjacency, jnp.mean(degree)


def setup_inputs(seed: int = 0) -> dict:
    key_mask, key_adj, key_feat, key_one, key_two = jax.random.split(jax.random.key(seed), 5)
    block_mask = draw_mask(key_mask)
    adjacency, mean_degree = build_adjacency(key_adj, block_mask)
    features = jax.random.normal(key_feat, (NODES, F0), jnp.float32).astype(jnp.bfloat16)
    w_one = (jax.random.normal(key_one, (F0, F1), jnp.float32) * jnp.sqrt(mean_degree / F0)).astype(jnp.bfloat16)
    w_two = (jax.random.normal(key_two, (F1, F2), jnp.float32) * (F1 ** -0.5)).astype(jnp.bfloat16)
    return {'adjacency': adjacency, 'block_mask': block_mask, 'features': features, 'w_one': w_one, 'w_two': w_two}


def reference(adjacency, block_mask, features, w_one, w_two):
    adj_blocks = adjacency.reshape(ROWS, BLOCK, NODES)

    def aggregate(feat_table):
        feat_width = feat_table.shape[1]
        feat_blocks = feat_table.reshape(ROWS, BLOCK, feat_width)

        def one_block(block_pair):
            adj_rows, mask_row = block_pair
            masked = (feat_blocks * mask_row.astype(feat_table.dtype)[:, None, None]).reshape(NODES, feat_width)
            return jnp.dot(adj_rows, masked, preferred_element_type=jnp.float32)

        return lax.map(one_block, (adj_blocks, block_mask)).reshape(NODES, feat_width)

    y_one = aggregate(features).astype(jnp.bfloat16)
    z_one = jnp.maximum(jnp.dot(y_one, w_one, preferred_element_type=jnp.float32), 0.0).astype(jnp.bfloat16)
    y_two = aggregate(z_one).astype(jnp.bfloat16)
    return jnp.dot(y_two, w_two, preferred_element_type=jnp.float32)
```

```python
import functools

import jax
import jax.numpy as jnp
from jax import lax
from jax.experimental import pallas as pl
from jax.experimental.pallas import tpu as pltpu
from jax.sharding import PartitionSpec as P

MESH = pl.DeviceIdType.MESH
BF16 = jnp.bfloat16
F32 = jnp.float32
SUB = 64
OUT_COLS = 128
S_LAG, OS_LAG, OF_LAG = 4, 12, 16


def dot(a, b, dims):
    return lax.dot_general(a, b, (dims, ((), ())), preferred_element_type=F32)


def kernel(mask_ref, adj_hbm, featt_ref, w1_ref, w2t_ref, outt_ref,
           adj, ht, w1p, w2p, pbuf, dbuf, xbuf, ybuf, yt, zt, y2, r_first, r_second, ot,
           adj_sem, ds_sem, dr_sem, xs_sem, xr_sem, ys_sem, yr_sem,
           gs_sem, gr_sem, fs_sem, fr_sem, ss_sem, sr_sem, us_sem, ur_sem, vs_sem, vr_sem):
    f0 = featt_ref.shape[0]
    f2 = w2t_ref.shape[0]
    f0p = ht.shape[0]
    f0s = pbuf.shape[2]
    blk, width = adj.shape
    chunk = width // 8
    half = chunk // 2
    rows_half = blk // 2
    mm_rows = blk // 8
    n_sub = rows_half // SUB
    sub_mm = mm_rows // SUB
    n_out = rows_half // OUT_COLS
    out_sub = OUT_COLS // SUB

    z = lax.axis_index('rep')
    r = lax.axis_index('rows')
    c = lax.rem(r, 2)
    x = lax.rem(r // 2, 2)
    y = r // 4
    core_p = r + 1 - 2 * c
    x_p = r + 2 - 4 * x
    y_p = r + 4 - 8 * y

    def rows_dev(i):
        return {'rows': i, 'rep': z}

    def rep_dev(i):
        return {'rows': r, 'rep': i}

    def order(k):
        ky, kx = lax.rem(k, 2), k // 2
        cy = y * ky + (1 - y) * (1 - ky)
        cx = x * kx + (1 - x) * (1 - kx)
        return 4 * cy + 2 * cx

    def chunk_of(s):
        side = s // 4
        return order(lax.rem(s, 4)) + (1 - c) * (1 - side) + c * side

    def chunk_cols(q):
        return pl.ds(pl.multiple_of(q * chunk, 128), chunk)

    def adj_copy(s):
        cols = chunk_cols(chunk_of(s))
        return pltpu.make_async_copy(adj_hbm.at[:, cols], adj.at[:, cols], adj_sem.at[s])

    for s in range(3):
        adj_copy(s).start()

    barrier = pltpu.get_barrier_semaphore()
    for dev in (core_p, x_p, y_p):
        pl.semaphore_signal(barrier, inc=1, device_id=rows_dev(dev), device_id_type=MESH)
    for dev in (lax.rem(z + 1, 4), lax.rem(z + 3, 4)):
        pl.semaphore_signal(barrier, inc=1, device_id=rep_dev(dev), device_id_type=MESH)

    ht[...] = jnp.zeros_like(ht)
    ht[0:f0, :] = featt_ref[...]
    w1p[...] = jnp.zeros_like(w1p)
    w1p[0:f0, :] = w1_ref[...]
    w2p[...] = jnp.zeros_like(w2p)
    w2p[0:f2, :] = w2t_ref[...]

    pl.semaphore_wait(barrier, 5)

    def remote(src, dst, send, recv, dev):
        return pltpu.make_async_remote_copy(
            src_ref=src, dst_ref=dst, send_sem=send, recv_sem=recv, device_id=dev, device_id_type=MESH)

    def core_copy(k):
        return remote(pbuf.at[k], dbuf.at[k], ds_sem.at[k], dr_sem.at[k], rows_dev(core_p))

    def x_copy(k, src):
        return remote(src, xbuf.at[k], xs_sem.at[k], xr_sem.at[k], rows_dev(x_p))

    def y_copy(k, src):
        return remote(src, ybuf.at[k], ys_sem.at[k], yr_sem.at[k], rows_dev(y_p))

    def layer_one(s, carry):
        q = chunk_of(s)
        adj_copy(s).wait()

        @pl.when(s < 5)
        def _():
            adj_copy(s + 3).start()

        keep = mask_ref[r, 2 * z + q // 4].astype(F32)
        part = dot(ht[...], adj[:, chunk_cols(q)], ((1,), (0,)))[0:f0s, :] * keep
        pbuf[s, 0] = part[:, 0:half]
        pbuf[s, 1] = part[:, half:chunk]

        @pl.when(s < 4)
        def _():
            core_copy(s).start()

        @pl.when(s >= 4)
        def _():
            core_copy(s - 4).wait_recv()
            pbuf[s] = pbuf[s] + dbuf[s - 4]

        @pl.when(s == 4)
        def _():
            x_copy(0, pbuf.at[4, 0]).start()
            y_copy(0, pbuf.at[4, 1]).start()

        @pl.when(s == 5)
        def _():
            x_copy(1, pbuf.at[5, 0]).start()

        @pl.when(s == 6)
        def _():
            y_copy(1, pbuf.at[6, 1]).start()

        return carry

    lax.fori_loop(0, 8, layer_one, 0)

    y_copy(0, pbuf.at[4, 1]).wait_recv()
    pbuf[5, 1] = pbuf[5, 1] + ybuf[0]
    x_copy(2, pbuf.at[5, 1]).start()
    x_copy(0, pbuf.at[4, 0]).wait_recv()
    pbuf[6, 0] = pbuf[6, 0] + xbuf[0]
    y_copy(2, pbuf.at[6, 0]).start()
    x_copy(1, pbuf.at[5, 0]).wait_recv()
    y_copy(1, pbuf.at[6, 1]).wait_recv()
    pbuf[7, 0] = pbuf[7, 0] + xbuf[1]
    pbuf[7, 1] = pbuf[7, 1] + ybuf[1]
    pad = jnp.zeros((f0p - f0s, half), F32)

    def own_cols(q, h):
        return pl.ds(pl.multiple_of(q * chunk + h * half, 128), half)

    x_copy(2, pbuf.at[5, 1]).wait_recv()
    yt[:, own_cols(r, 1)] = jnp.concatenate([pbuf[7, 1] + xbuf[2], pad], axis=0).astype(BF16)
    y_copy(2, pbuf.at[6, 0]).wait_recv()
    yt[:, own_cols(r, 0)] = jnp.concatenate([pbuf[7, 0] + ybuf[2], pad], axis=0).astype(BF16)

    diag = y_p + x_p - r

    def whole(q):
        return yt.at[:, chunk_cols(q)]

    def part_of(q, h):
        return yt.at[:, own_cols(q, h)]

    def gather_copy(k, ref, dev):
        return remote(ref, ref, gs_sem.at[k], gr_sem.at[k], rows_dev(dev))

    def relu_rows(q):
        cols = chunk_cols(q)
        keep = mask_ref[r, 2 * z + q // 4].astype(F32)
        rows = dot(yt[:, cols], w1p[...], ((0,), (0,)))
        zt[cols, :] = (jnp.maximum(rows, 0.0) * keep).astype(BF16)

    gather_copy(0, whole(r), x_p).start()
    gather_copy(1, whole(r), y_p).start()
    gather_copy(2, whole(r), core_p).start()
    relu_rows(r)
    gather_copy(2, whole(core_p), core_p).wait_recv()
    relu_rows(core_p)
    gather_copy(0, whole(x_p), x_p).wait_recv()
    gather_copy(3, part_of(x_p, 1), y_p).start()
    gather_copy(4, whole(x_p), core_p).start()
    gather_copy(1, whole(y_p), y_p).wait_recv()
    gather_copy(5, part_of(y_p, 0), x_p).start()
    gather_copy(6, whole(y_p), core_p).start()
    relu_rows(x_p)
    relu_rows(y_p)
    other = 1 - 2 * c
    gather_copy(4, whole(x_p + other), core_p).wait_recv()
    relu_rows(x_p + other)
    gather_copy(6, whole(y_p + other), core_p).wait_recv()
    relu_rows(y_p + other)
    gather_copy(3, part_of(diag, 1), y_p).wait_recv()
    gather_copy(5, part_of(diag, 0), x_p).wait_recv()
    gather_copy(7, whole(diag), core_p).start()
    relu_rows(diag)
    gather_copy(7, whole(diag + other), core_p).wait_recv()
    relu_rows(diag + other)

    low = z // 2
    step = 1 - 2 * low
    first_off = low * rows_half
    second_off = rows_half - first_off
    inner = rep_dev(lax.rem(z + step + 4, 4))
    outer = rep_dev(lax.rem(z - step + 4, 4))
    is_end = lax.rem(z, 3) == 0
    is_mid = lax.rem(z, 3) != 0

    def rows_at(off, n, size):
        return pl.ds(pl.multiple_of(off + n * size, 64), size)

    def first_rows(u):
        return rows_at(first_off, u, SUB)

    def second_rows(u):
        return rows_at(second_off, u, SUB)

    def slot(u):
        return rows_at(0, u, SUB)

    def first_end(u):
        return remote(y2.at[first_rows(u)], r_first.at[slot(u)], fs_sem.at[u], fr_sem.at[u], inner)

    def first_mid(u):
        return remote(y2.at[first_rows(u)], r_second.at[slot(u)], fs_sem.at[u], sr_sem.at[u], inner)

    def second_mid(u):
        return remote(y2.at[second_rows(u)], r_second.at[slot(u)], ss_sem.at[u], sr_sem.at[u], outer)

    def second_out(v):
        return ot.at[:, pl.ds(pl.multiple_of(second_off + v * OUT_COLS, 128), OUT_COLS)]

    def first_out(v):
        return ot.at[:, pl.ds(pl.multiple_of(first_off + v * OUT_COLS, 128), OUT_COLS)]

    def out_end(v):
        return remote(second_out(v), second_out(v), us_sem.at[v], ur_sem.at[v], inner)

    def out_mid(v):
        return remote(second_out(v), second_out(v), us_sem.at[v], vr_sem.at[v], inner)

    def out_last(v):
        return remote(first_out(v), first_out(v), vs_sem.at[v], vr_sem.at[v], outer)

    def event(it, carry):
        t = it - 4
        late = (t >= 2) & (t <= 11) & (lax.rem(t + 1, 3) == 0)

        @pl.when((it < 4) | late)
        def _():
            mi = jnp.where(it < 4, it, 4 + t // 3)
            is_second = (mi == 1) | (mi == 4) | (mi >= 6)
            m = jnp.where(mi == 1, 0, jnp.where(mi == 2, 1, jnp.where(mi == 3, 2, jnp.where(
                mi == 4, 1, jnp.where(mi == 5, 3, jnp.where(mi == 6, 2, jnp.where(mi == 7, 3, 0)))))))
            off = jnp.where(is_second, second_off, first_off)
            rows = rows_at(off, m, mm_rows)
            y2[rows, :] = dot(adj[rows, :], zt[...], ((1,), (0,)))

            @pl.when(is_end & jnp.logical_not(is_second))
            def _():
                def send(u, carry):
                    first_end(m * sub_mm + u).start()
                    return carry

                lax.fori_loop(0, sub_mm, send, 0)

        @pl.when(is_mid & (t >= 0) & (t < n_sub))
        def _():
            u = t
            first_end(u).wait_recv()
            y2[first_rows(u), :] = y2[first_rows(u), :] + r_first[slot(u), :]
            first_mid(u).start()

        @pl.when(is_mid & (t >= S_LAG) & (t < n_sub + S_LAG))
        def _():
            u = t - S_LAG
            first_mid(u).wait_recv()
            y2[second_rows(u), :] = y2[second_rows(u), :] + r_second[slot(u), :]
            second_mid(u).start()

        @pl.when(is_mid & (t >= OS_LAG) & (t < n_sub + OS_LAG) & (lax.rem(t - OS_LAG + 64, out_sub) == 0))
        def _():
            v = (t - OS_LAG) // out_sub
            out_end(v).wait_recv()
            out_mid(v).start()

        @pl.when(is_mid & (t >= OF_LAG) & (t < n_sub + OF_LAG) & (lax.rem(t - OF_LAG + 64, out_sub) == 0))
        def _():
            v = (t - OF_LAG) // out_sub
            out_mid(v).wait_recv()
            out_last(v).start()

        @pl.when(is_end & (t >= 12) & (t < n_sub + 12) & (lax.rem(t - 12 + 64, out_sub) == out_sub - 1))
        def _():
            v = (t - 12) // out_sub
            for i in range(out_sub):
                second_mid(v * out_sub + i).wait_recv()
            rows = rows_at(second_off, v, OUT_COLS)
            total = (y2[rows, :] + r_second[rows_at(0, v, OUT_COLS), :]).astype(BF16)
            second_out(v)[...] = dot(w2p[...], total, ((1,), (1,)))
            out_end(v).start()

        return carry

    lax.fori_loop(0, n_sub + OF_LAG + 4, event, 0)

    for k in range(4):
        core_copy(k).wait_send()
    x_copy(0, pbuf.at[4, 0]).wait_send()
    x_copy(1, pbuf.at[5, 0]).wait_send()
    x_copy(2, pbuf.at[5, 1]).wait_send()
    y_copy(0, pbuf.at[4, 1]).wait_send()
    y_copy(1, pbuf.at[6, 1]).wait_send()
    y_copy(2, pbuf.at[6, 0]).wait_send()
    for k, ref in ((0, whole(r)), (1, whole(r)), (2, whole(r)), (3, part_of(x_p, 1)), (4, whole(x_p)),
                   (5, part_of(y_p, 0)), (6, whole(y_p)), (7, whole(diag))):
        gather_copy(k, ref, core_p).wait_send()

    def drain_sub(u, carry):
        @pl.when(is_end)
        def _():
            first_end(u).wait_send()

        @pl.when(is_mid)
        def _():
            first_mid(u).wait_send()
            second_mid(u).wait_send()

        return carry

    lax.fori_loop(0, n_sub, drain_sub, 0)

    def drain_out(v, carry):
        @pl.when(is_end)
        def _():
            out_last(v).wait_recv()
            out_end(v).wait_send()

        @pl.when(is_mid)
        def _():
            out_mid(v).wait_send()
            out_last(v).wait_send()

        return carry

    lax.fori_loop(0, n_out, drain_out, 0)
    outt_ref[...] = ot[0:f2, :]


def solution(mesh):
    def local_fn(adj_local, block_mask, feat_blk, w_one, w_two):
        blk, width = adj_local.shape
        f0, f1 = w_one.shape
        f2 = w_two.shape[1]
        f0s = -(-f0 // 8) * 8
        f0p = -(-f0 // 16) * 16
        f2p = -(-f2 // 16) * 16
        chunk, rows_half = width // 8, blk // 2
        half = chunk // 2
        n_sub, n_out = rows_half // SUB, rows_half // OUT_COLS
        vmem = pl.BlockSpec(memory_space=pltpu.VMEM)
        dma = pltpu.SemaphoreType.DMA
        outt = pl.pallas_call(
            kernel,
            out_shape=jax.ShapeDtypeStruct((f2, blk), F32),
            in_specs=[pl.BlockSpec(memory_space=pltpu.SMEM), pl.BlockSpec(memory_space=pl.ANY), vmem, vmem, vmem],
            out_specs=vmem,
            scratch_shapes=[
                pltpu.VMEM((blk, width), BF16),
                pltpu.VMEM((f0p, blk), BF16),
                pltpu.VMEM((f0p, f1), BF16),
                pltpu.VMEM((f2p, f1), BF16),
                pltpu.VMEM((8, 2, f0s, half), F32),
                pltpu.VMEM((4, 2, f0s, half), F32),
                pltpu.VMEM((3, f0s, half), F32),
                pltpu.VMEM((3, f0s, half), F32),
                pltpu.VMEM((f0p, width), BF16),
                pltpu.VMEM((width, f1), BF16),
                pltpu.VMEM((blk, f1), F32),
                pltpu.VMEM((rows_half, f1), F32),
                pltpu.VMEM((rows_half, f1), F32),
                pltpu.VMEM((f2p, blk), F32),
                dma((8,)),
                dma((4,)), dma((4,)),
                dma((3,)), dma((3,)), dma((3,)), dma((3,)),
                dma((8,)), dma((8,)),
                dma((n_sub,)), dma((n_sub,)), dma((n_sub,)), dma((n_sub,)),
                dma((n_out,)), dma((n_out,)), dma((n_out,)), dma((n_out,)),
            ],
            compiler_params=pltpu.CompilerParams(collective_id=0, has_side_effects=True, vmem_limit_bytes=63 * 1024 * 1024),
        )(block_mask, adj_local, feat_blk.T, w_one, w_two.T)
        return outt.T

    return jax.shard_map(local_fn, mesh=mesh, in_specs=(P('rows', 'rep'), P(), P('rows', None), P(), P()), out_specs=P('rows', None), check_vma=False)
```

```python
import jax
import jax.numpy as jnp
from jax import lax
from jax.experimental import pallas as pl
from jax.experimental.pallas import tpu as pltpu
from jax.sharding import PartitionSpec as P

MESH = pl.DeviceIdType.MESH
BF16 = jnp.bfloat16
F32 = jnp.float32
SUB = 64
OUT_COLS = 128
AHEAD = 4
LEAD = 5
S_LAG = 4
END_LAG = 12


def dot(a, b, dims):
    return lax.dot_general(a, b, (dims, ((), ())), preferred_element_type=F32)


def scope(name):
    return jax.named_scope(name)


def kernel(mask_ref, adj_hbm, featt_hbm, w1_hbm, w2t_hbm, out_hbm,
           adj, featt, w1, w2t, ht, w1p, w2p, abuf, dbuf, xbuf, ybuf, yt, zt, y2, r_first, r_second, ot,
           adj_sem, in_sem, ds_sem, dr_sem, xs_sem, xr_sem, ys_sem, yr_sem,
           gs_sem, gr_sem, fs_sem, fr_sem, ss_sem, sr_sem, us_sem, ur_sem, vs_sem, vr_sem, o_sem):
    f0, f2 = featt.shape[0], w2t.shape[0]
    f0p, f0s = ht.shape[0], abuf.shape[2]
    blk, width = adj.shape
    piece = abuf.shape[3]
    block = 2 * piece
    rows_half = blk // 2
    mm_rows = blk // 16
    n_sub = rows_half // SUB
    sub_mm = mm_rows // SUB
    n_out = rows_half // OUT_COLS
    out_sub = OUT_COLS // SUB

    z = lax.axis_index('rep')
    r = lax.axis_index('rows')
    c = lax.rem(r, 2)
    x = lax.rem(r // 2, 2)
    y = r // 4
    core_p = r + 1 - 2 * c
    x_p = r + 2 - 4 * x
    y_p = r + 4 - 8 * y

    low = z // 2
    step = 1 - 2 * low
    inner_z = lax.rem(z + step + 4, 4)
    outer_z = lax.rem(z - step + 4, 4)
    is_end = lax.rem(z, 3) == 0
    is_mid = lax.rem(z, 3) != 0

    def rows_dev(i):
        return {'rows': i, 'rep': z}

    inner, outer = {'rows': r, 'rep': inner_z}, {'rows': r, 'rep': outer_z}

    def group(k):
        ky, kx = lax.rem(k, 2), k // 2
        cy = y * ky + (1 - y) * (1 - ky)
        cx = x * kx + (1 - x) * (1 - kx)
        return 2 * cy + cx

    def block_of(p):
        k = jnp.where(p < 2, 0, jnp.where(p >= 6, 3, jnp.where((p == 2) | (p == 4), 1, 2)))
        h = jnp.where((p == 0) | (p == 2) | (p == 5) | (p == 6), 0, 1)
        return 2 * group(k) + h

    def block_cols(b):
        return pl.ds(pl.multiple_of(b * block, 128), block)

    def adj_copy(p):
        cols = block_cols(block_of(p))
        return pltpu.make_async_copy(adj_hbm.at[:, cols], adj.at[:, cols], adj_sem.at[p])

    in_copies = [pltpu.make_async_copy(src, dst, in_sem.at[i])
                 for i, (src, dst) in enumerate(((featt_hbm, featt), (w1_hbm, w1), (w2t_hbm, w2t)))]
    in_copies[0].start()
    for p in range(AHEAD):
        adj_copy(p).start()
    in_copies[1].start()
    in_copies[2].start()

    barrier = pltpu.get_barrier_semaphore()
    for dev in (core_p, x_p, y_p):
        pl.semaphore_signal(barrier, inc=1, device_id=rows_dev(dev), device_id_type=MESH)
    pl.semaphore_signal(barrier, inc=1, device_id=inner, device_id_type=MESH)

    @pl.when(is_mid)
    def _():
        pl.semaphore_signal(barrier, inc=1, device_id=outer, device_id_type=MESH)

    ht[...] = jnp.zeros_like(ht)
    w1p[...] = jnp.zeros_like(w1p)
    w2p[...] = jnp.zeros_like(w2p)
    in_copies[0].wait()
    ht[0:f0, :] = featt[...]
    in_copies[1].wait()
    w1p[0:f0, :] = w1[...]
    in_copies[2].wait()
    w2p[0:f2, :] = w2t[...]

    with scope('barrier'):
        pl.semaphore_wait(barrier, jnp.where(is_end, 4, 5))

    def remote(src, dst, send, recv, dev):
        return pltpu.make_async_remote_copy(
            src_ref=src, dst_ref=dst, send_sem=send, recv_sem=recv, device_id=dev, device_id_type=MESH)

    def core_copy(p):
        return remote(abuf.at[p, 1 - c], dbuf.at[p], ds_sem.at[p], dr_sem.at[p], rows_dev(core_p))

    def x_copy(k, p):
        return remote(abuf.at[p, c], xbuf.at[k], xs_sem.at[k], xr_sem.at[k], rows_dev(x_p))

    def y_copy(k, p):
        return remote(abuf.at[p, c], ybuf.at[k], ys_sem.at[k], yr_sem.at[k], rows_dev(y_p))

    def layer_one(p, carry):
        @pl.when(p < 8)
        def _():
            b = block_of(p)
            with scope('adj_wait'):
                adj_copy(p).wait()

            @pl.when(p < 8 - AHEAD)
            def _():
                adj_copy(p + AHEAD).start()

            keep = mask_ref[r, 2 * z + b // 4].astype(F32)
            part = dot(ht[...], adj[:, block_cols(b)], ((1,), (0,)))[0:f0s, :] * keep
            abuf[p, 0] = part[:, 0:piece]
            abuf[p, 1] = part[:, piece:block]
            core_copy(p).start()

        @pl.when(p >= 1)
        def _():
            with scope('core_add'):
                core_copy(p - 1).wait_recv()
                abuf[p - 1, c] = abuf[p - 1, c] + dbuf[p - 1]

        @pl.when(p == 1)
        def _():
            x_copy(0, 0).start()

        @pl.when(p == 2)
        def _():
            y_copy(0, 1).start()

        @pl.when(p == 3)
        def _():
            x_copy(1, 2).start()

        @pl.when(p == 4)
        def _():
            y_copy(1, 3).start()

        return carry

    with scope('l1'):
        lax.fori_loop(0, 8, layer_one, 0)

    with scope('rs0'):
        y_copy(0, 1).wait_recv()
        abuf[4, c] = abuf[4, c] + ybuf[0]
        x_copy(2, 4).start()
    with scope('rs1'):
        x_copy(0, 0).wait_recv()
        abuf[5, c] = abuf[5, c] + xbuf[0]
        y_copy(2, 5).start()
    with scope('rs2'):
        core_copy(7).wait_recv()
        abuf[7, c] = abuf[7, c] + dbuf[7]
    with scope('rs3'):
        y_copy(1, 3).wait_recv()
        abuf[7, c] = abuf[7, c] + ybuf[1]
        x_copy(1, 2).wait_recv()
        abuf[6, c] = abuf[6, c] + xbuf[1]

    own_g, x_g, y_g, diag_g = r // 2, x_p // 2, y_p // 2, y_p // 2 + x_p // 2 - r // 2
    pad = jnp.zeros((f0p - f0s, piece), F32)

    def cols_of(g, h, cc):
        return pl.ds(pl.multiple_of((2 * g + h) * block + cc * piece, 128), piece)

    def gather_copy(k, g, h, dev, cc=None):
        ref = yt.at[:, cols_of(g, h, c if cc is None else cc)]
        return remote(ref, ref, gs_sem.at[k], gr_sem.at[k], rows_dev(dev))

    def core_recv(k, g, h):
        gather_copy(k, g, h, core_p, 1 - c).wait_recv()

    def relu_rows(g, h):
        cols = block_cols(2 * g + h)
        keep = mask_ref[r, 2 * z + g // 2].astype(F32)
        rows = dot(yt[:, cols], w1p[...], ((0,), (0,)))
        zt[cols, :] = (jnp.maximum(rows, 0.0) * keep).astype(BF16)

    with scope('rs4'):
        x_copy(2, 4).wait_recv()
        yt[:, cols_of(own_g, 1, c)] = jnp.concatenate([abuf[7, c] + xbuf[2], pad], axis=0).astype(BF16)
        gather_copy(0, own_g, 1, x_p).start()
        gather_copy(7, own_g, 1, core_p).start()
    with scope('rs5'):
        y_copy(2, 5).wait_recv()
        yt[:, cols_of(own_g, 0, c)] = jnp.concatenate([abuf[6, c] + ybuf[2], pad], axis=0).astype(BF16)
        gather_copy(2, own_g, 0, y_p).start()
        gather_copy(1, own_g, 0, x_p).start()
        gather_copy(3, own_g, 1, y_p).start()
        gather_copy(6, own_g, 0, core_p).start()
    with scope('g0'):
        core_recv(7, own_g, 1)
        relu_rows(own_g, 1)
        core_recv(6, own_g, 0)
        relu_rows(own_g, 0)
    with scope('g1'):
        gather_copy(0, x_g, 1, x_p).wait_recv()
        gather_copy(5, x_g, 1, y_p).start()
        gather_copy(8, x_g, 1, core_p).start()
    with scope('g2'):
        gather_copy(2, y_g, 0, y_p).wait_recv()
        gather_copy(4, y_g, 0, x_p).start()
        gather_copy(10, y_g, 0, core_p).start()
    with scope('g3'):
        core_recv(8, x_g, 1)
        relu_rows(x_g, 1)
        core_recv(10, y_g, 0)
        relu_rows(y_g, 0)
    with scope('g4'):
        gather_copy(1, x_g, 0, x_p).wait_recv()
        gather_copy(9, x_g, 0, core_p).start()
        gather_copy(3, y_g, 1, y_p).wait_recv()
        gather_copy(11, y_g, 1, core_p).start()
    with scope('g5'):
        core_recv(9, x_g, 0)
        relu_rows(x_g, 0)
        core_recv(11, y_g, 1)
        relu_rows(y_g, 1)
    with scope('g6'):
        gather_copy(4, diag_g, 0, x_p).wait_recv()
        gather_copy(12, diag_g, 0, core_p).start()
        gather_copy(5, diag_g, 1, y_p).wait_recv()
        gather_copy(13, diag_g, 1, core_p).start()
    with scope('g7'):
        core_recv(12, diag_g, 0)
        relu_rows(diag_g, 0)
        core_recv(13, diag_g, 1)
        relu_rows(diag_g, 1)

    first_off = low * rows_half
    second_off = rows_half - first_off

    def rows_at(off, n, size):
        return pl.ds(pl.multiple_of(off + n * size, SUB), size)

    def first_rows(u):
        return rows_at(first_off, u, SUB)

    def second_rows(u):
        return rows_at(second_off, u, SUB)

    def slot(u):
        return rows_at(0, u, SUB)

    def first_end(u):
        return remote(y2.at[first_rows(u)], r_first.at[slot(u)], fs_sem.at[u], fr_sem.at[u], inner)

    def first_mid(u):
        return remote(y2.at[first_rows(u)], r_second.at[slot(u)], fs_sem.at[u], sr_sem.at[u], inner)

    def second_mid(u):
        return remote(y2.at[second_rows(u)], r_second.at[slot(u)], ss_sem.at[u], sr_sem.at[u], outer)

    def out_cols(off, v):
        return pl.ds(pl.multiple_of(off + v * OUT_COLS, 128), OUT_COLS)

    def second_out(v):
        return ot.at[:, out_cols(second_off, v)]

    def first_out(v):
        return ot.at[:, out_cols(first_off, v)]

    def out_end(v):
        return remote(second_out(v), second_out(v), us_sem.at[v], ur_sem.at[v], inner)

    def out_mid(v):
        return remote(second_out(v), second_out(v), us_sem.at[v], vr_sem.at[v], inner)

    def out_last(v):
        return remote(first_out(v), first_out(v), vs_sem.at[v], vr_sem.at[v], outer)

    def save_second(v):
        return pltpu.make_async_copy(second_out(v), out_hbm.at[:, out_cols(second_off, v)], o_sem.at[0, v])

    def save_first(v):
        return pltpu.make_async_copy(first_out(v), out_hbm.at[:, out_cols(first_off, v)], o_sem.at[1, v])

    def event(it, carry):
        t = it - LEAD

        @pl.when(it < 16)
        def _():
            is_second, m = lax.rem(it, 2), it // 2
            off = first_off + is_second * (second_off - first_off)
            rows = rows_at(off, m, mm_rows)
            with scope('mm2'):
                y2[rows, :] = dot(adj[rows, :], zt[...], ((1,), (0,)))

            @pl.when(is_end & (is_second == 0))
            def _():
                for u in range(sub_mm):
                    first_end(m * sub_mm + u).start()

        @pl.when(is_mid & (t >= 0) & (t < n_sub))
        def _():
            with scope('wF'):
                first_end(t).wait_recv()
            y2[first_rows(t), :] = y2[first_rows(t), :] + r_first[slot(t), :]
            first_mid(t).start()

        @pl.when(is_mid & (t >= S_LAG) & (t < n_sub + S_LAG))
        def _():
            u = t - S_LAG
            with scope('wS'):
                first_mid(u).wait_recv()
            y2[second_rows(u), :] = y2[second_rows(u), :] + r_second[slot(u), :]
            second_mid(u).start()

        @pl.when(is_end & (t >= END_LAG) & (t < n_sub + END_LAG) & (lax.rem(t - END_LAG + 64, out_sub) == out_sub - 1))
        def _():
            v = (t - END_LAG) // out_sub
            with scope('wE'):
                for i in range(out_sub):
                    second_mid(v * out_sub + i).wait_recv()
            rows = rows_at(second_off, v, OUT_COLS)
            total = (y2[rows, :] + r_second[rows_at(0, v, OUT_COLS), :]).astype(BF16)
            second_out(v)[...] = dot(w2p[...], total, ((1,), (1,)))[0:f2, :]
            out_end(v).start()
            save_second(v).start()

        return carry

    lax.fori_loop(0, n_sub + END_LAG + LEAD, event, 0)

    def pass_on(v, carry):
        @pl.when(is_mid)
        def _():
            with scope('wOS'):
                out_end(v).wait_recv()
            out_mid(v).start()
            save_second(v).start()
            with scope('wOF'):
                out_mid(v).wait_recv()
            out_last(v).start()
            save_first(v).start()

        @pl.when(is_end)
        def _():
            with scope('wOE'):
                out_last(v).wait_recv()
            save_first(v).start()

        return carry

    lax.fori_loop(0, n_out, pass_on, 0)

    with scope('drain'):
        for p in range(8):
            core_copy(p).wait_send()
        x_copy(0, 0).wait_send()
        x_copy(1, 2).wait_send()
        x_copy(2, 4).wait_send()
        y_copy(0, 1).wait_send()
        y_copy(1, 3).wait_send()
        y_copy(2, 5).wait_send()
        for k in range(14):
            gather_copy(k, own_g, 0, core_p).wait_send()

        def drain_sub(u, carry):
            first_end(u).wait_send()

            @pl.when(is_mid)
            def _():
                second_mid(u).wait_send()

            return carry

        lax.fori_loop(0, n_sub, drain_sub, 0)

        def drain_out(v, carry):
            out_end(v).wait_send()

            @pl.when(is_mid)
            def _():
                out_last(v).wait_send()

            save_first(v).wait()
            save_second(v).wait()
            return carry

        lax.fori_loop(0, n_out, drain_out, 0)


def solution(mesh):
    def local_fn(adj_local, block_mask, feat_blk, w_one, w_two):
        blk, width = adj_local.shape
        f0, f1 = w_one.shape
        f2 = w_two.shape[1]
        f0s = -(-f0 // 8) * 8
        f0p = -(-f0 // 16) * 16
        f2p = -(-f2 // 16) * 16
        piece, rows_half = width // 16, blk // 2
        n_sub, n_out = rows_half // SUB, rows_half // OUT_COLS
        hbm = pl.BlockSpec(memory_space=pl.ANY)
        dma = pltpu.SemaphoreType.DMA
        outt = pl.pallas_call(
            kernel,
            out_shape=jax.ShapeDtypeStruct((f2, blk), F32),
            in_specs=[pl.BlockSpec(memory_space=pltpu.SMEM), hbm, hbm, hbm, hbm],
            out_specs=hbm,
            scratch_shapes=[
                pltpu.VMEM((blk, width), BF16),
                pltpu.VMEM((f0, blk), BF16),
                pltpu.VMEM((f0, f1), BF16),
                pltpu.VMEM((f2, f1), BF16),
                pltpu.VMEM((f0p, blk), BF16),
                pltpu.VMEM((f0p, f1), BF16),
                pltpu.VMEM((f2p, f1), BF16),
                pltpu.VMEM((8, 2, f0s, piece), F32),
                pltpu.VMEM((8, f0s, piece), F32),
                pltpu.VMEM((3, f0s, piece), F32),
                pltpu.VMEM((3, f0s, piece), F32),
                pltpu.VMEM((f0p, width), BF16),
                pltpu.VMEM((width, f1), BF16),
                pltpu.VMEM((blk, f1), F32),
                pltpu.VMEM((rows_half, f1), F32),
                pltpu.VMEM((rows_half, f1), F32),
                pltpu.VMEM((f2, blk), F32),
                dma((8,)), dma((3,)),
                dma((8,)), dma((8,)),
                dma((3,)), dma((3,)), dma((3,)), dma((3,)),
                dma((14,)), dma((14,)),
                dma((n_sub,)), dma((n_sub,)), dma((n_sub,)), dma((n_sub,)),
                dma((n_out,)), dma((n_out,)), dma((n_out,)), dma((n_out,)),
                dma((2, n_out)),
            ],
            compiler_params=pltpu.CompilerParams(collective_id=0, has_side_effects=True, vmem_limit_bytes=63 * 1024 * 1024),
        )(block_mask, adj_local, feat_blk.T, w_one, w_two.T)
        return outt.T

    return jax.shard_map(local_fn, mesh=mesh, in_specs=(P('rows', 'rep'), P(), P('rows', None), P(), P()), out_specs=P('rows', None), check_vma=False)
```

```python
import jax
import jax.numpy as jnp
from jax import lax
from jax.experimental import pallas as pl
from jax.experimental.pallas import tpu as pltpu
from jax.sharding import PartitionSpec as P

MESH = pl.DeviceIdType.MESH
BF16 = jnp.bfloat16
F32 = jnp.float32
SUB = 64
OUT_COLS = 128
LEAD = 5
S_LAG = 4
END_LAG = 12
OUT_LAG = 4
DIRECT = 2


def dot(a, b, dims):
    return lax.dot_general(a, b, (dims, ((), ())), preferred_element_type=F32)


def scope(name):
    return jax.named_scope(name)


def kernel(mask_ref, adj_hbm, featt_hbm, w1_hbm, w2t_hbm, out_hbm,
           adj, featt, w1, w2t, ht, w1p, w2p, abuf, dbuf, xbuf, ybuf, yt, zt, y2, r_first, r_second, ot,
           adj_sem, in_sem, ds_sem, dr_sem, xs_sem, xr_sem, ys_sem, yr_sem,
           gs_sem, gr_sem, fs_sem, fr_sem, ss_sem, sr_sem, us_sem, ur_sem, vs_sem, vr_sem, o_sem):
    f0, f2 = featt.shape[0], w2t.shape[0]
    f0p, f0s = ht.shape[0], abuf.shape[2]
    blk, width = adj.shape
    piece = abuf.shape[3]
    block = 2 * piece
    rows_half = blk // 2
    mm_rows = blk // 16
    n_sub = rows_half // SUB
    sub_mm = mm_rows // SUB
    n_out = rows_half // OUT_COLS
    out_sub = OUT_COLS // SUB

    z = lax.axis_index('rep')
    r = lax.axis_index('rows')
    c = lax.rem(r, 2)
    x = lax.rem(r // 2, 2)
    y = r // 4
    core_p = r + 1 - 2 * c
    x_p = r + 2 - 4 * x
    y_p = r + 4 - 8 * y

    low = z // 2
    step = 1 - 2 * low
    inner_z = lax.rem(z + step + 4, 4)
    outer_z = lax.rem(z - step + 4, 4)
    is_end = lax.rem(z, 3) == 0
    is_mid = lax.rem(z, 3) != 0

    def rows_dev(i):
        return {'rows': i, 'rep': z}

    inner, outer = {'rows': r, 'rep': inner_z}, {'rows': r, 'rep': outer_z}

    def group(k):
        ky, kx = lax.rem(k, 2), k // 2
        cy = y * ky + (1 - y) * (1 - ky)
        cx = x * kx + (1 - x) * (1 - kx)
        return 2 * cy + cx

    def block_of(p):
        k = jnp.where(p < 2, 0, jnp.where(p >= 6, 3, jnp.where((p == 2) | (p == 4), 1, 2)))
        h = jnp.where((p == 0) | (p == 2) | (p == 5) | (p == 6), 0, 1)
        return 2 * group(k) + h

    def block_cols(b):
        return pl.ds(pl.multiple_of(b * block, 128), block)

    def adj_copy(p):
        cols = block_cols(block_of(p))
        return pltpu.make_async_copy(adj_hbm.at[:, cols], adj.at[:, cols], adj_sem.at[p])

    in_copies = [pltpu.make_async_copy(src, dst, in_sem.at[i])
                 for i, (src, dst) in enumerate(((featt_hbm, featt), (w1_hbm, w1), (w2t_hbm, w2t)))]
    for copy in in_copies:
        copy.start()
    for p in range(8):
        adj_copy(p).start()

    barrier = pltpu.get_barrier_semaphore()
    for dev in (core_p, x_p, y_p):
        pl.semaphore_signal(barrier, inc=1, device_id=rows_dev(dev), device_id_type=MESH)
    pl.semaphore_signal(barrier, inc=1, device_id=inner, device_id_type=MESH)

    @pl.when(is_mid)
    def _():
        pl.semaphore_signal(barrier, inc=1, device_id=outer, device_id_type=MESH)

    ht[...] = jnp.zeros_like(ht)
    w1p[...] = jnp.zeros_like(w1p)
    w2p[...] = jnp.zeros_like(w2p)
    in_copies[0].wait()
    ht[0:f0, :] = featt[...]
    in_copies[1].wait()
    w1p[0:f0, :] = w1[...]
    in_copies[2].wait()
    w2p[0:f2, :] = w2t[...]

    with scope('barrier'):
        pl.semaphore_wait(barrier, jnp.where(is_end, 4, 5))

    def remote(src, dst, send, recv, dev):
        return pltpu.make_async_remote_copy(
            src_ref=src, dst_ref=dst, send_sem=send, recv_sem=recv, device_id=dev, device_id_type=MESH)

    def core_copy(p):
        return remote(abuf.at[p, 1 - c], dbuf.at[p], ds_sem.at[0], dr_sem.at[p], rows_dev(core_p))

    def x_copy(k, p):
        return remote(abuf.at[p, c], xbuf.at[k], xs_sem.at[0], xr_sem.at[k], rows_dev(x_p))

    def y_copy(k, p):
        return remote(abuf.at[p, c], ybuf.at[k], ys_sem.at[0], yr_sem.at[k], rows_dev(y_p))

    def layer_one(p, carry):
        @pl.when(p < 8)
        def _():
            b = block_of(p)
            with scope('adj_wait'):
                adj_copy(p).wait()

            keep = mask_ref[r, 2 * z + b // 4].astype(F32)
            part = dot(ht[...], adj[:, block_cols(b)], ((1,), (0,)))[0:f0s, :] * keep
            abuf[p, 0] = part[:, 0:piece]
            abuf[p, 1] = part[:, piece:block]
            core_copy(p).start()

        @pl.when(p >= 1)
        def _():
            with scope('core_add'):
                core_copy(p - 1).wait_recv()
                abuf[p - 1, c] = abuf[p - 1, c] + dbuf[p - 1]

        @pl.when(p == 1)
        def _():
            x_copy(0, 0).start()

        @pl.when(p == 2)
        def _():
            y_copy(0, 1).start()

        @pl.when(p == 3)
        def _():
            x_copy(1, 2).start()

        @pl.when(p == 4)
        def _():
            y_copy(1, 3).start()

        return carry

    with scope('l1'):
        lax.fori_loop(0, 8, layer_one, 0)

    with scope('rs0'):
        y_copy(0, 1).wait_recv()
        abuf[4, c] = abuf[4, c] + ybuf[0]
        x_copy(2, 4).start()
    with scope('rs1'):
        x_copy(0, 0).wait_recv()
        abuf[5, c] = abuf[5, c] + xbuf[0]
        y_copy(2, 5).start()
    with scope('rs2'):
        core_copy(7).wait_recv()
        abuf[7, c] = abuf[7, c] + dbuf[7]
    with scope('rs3'):
        y_copy(1, 3).wait_recv()
        abuf[7, c] = abuf[7, c] + ybuf[1]
        x_copy(1, 2).wait_recv()
        abuf[6, c] = abuf[6, c] + xbuf[1]

    own_g, x_g, y_g, diag_g = r // 2, x_p // 2, y_p // 2, y_p // 2 + x_p // 2 - r // 2
    pad = jnp.zeros((f0p - f0s, piece), F32)

    def cols_of(g, h, cc):
        return pl.ds(pl.multiple_of((2 * g + h) * block + cc * piece, 128), piece)

    def gather_copy(k, g, h, dev, cc=None):
        ref = yt.at[:, cols_of(g, h, c if cc is None else cc)]
        return remote(ref, ref, gs_sem.at[0], gr_sem.at[k], rows_dev(dev))

    def core_recv(k, g, h):
        gather_copy(k, g, h, core_p, 1 - c).wait_recv()

    def relu_rows(g, h):
        cols = block_cols(2 * g + h)
        keep = mask_ref[r, 2 * z + g // 2].astype(F32)
        rows = dot(yt[:, cols], w1p[...], ((0,), (0,)))
        zt[cols, :] = (jnp.maximum(rows, 0.0) * keep).astype(BF16)

    with scope('rs4'):
        x_copy(2, 4).wait_recv()
        yt[:, cols_of(own_g, 1, c)] = jnp.concatenate([abuf[7, c] + xbuf[2], pad], axis=0).astype(BF16)
        gather_copy(0, own_g, 1, x_p).start()
        gather_copy(7, own_g, 1, core_p).start()
    with scope('rs5'):
        y_copy(2, 5).wait_recv()
        yt[:, cols_of(own_g, 0, c)] = jnp.concatenate([abuf[6, c] + ybuf[2], pad], axis=0).astype(BF16)
        gather_copy(2, own_g, 0, y_p).start()
        gather_copy(1, own_g, 0, x_p).start()
        gather_copy(3, own_g, 1, y_p).start()
        gather_copy(6, own_g, 0, core_p).start()
    with scope('g0'):
        core_recv(7, own_g, 1)
        relu_rows(own_g, 1)
        core_recv(6, own_g, 0)
        relu_rows(own_g, 0)
    with scope('g1'):
        gather_copy(0, x_g, 1, x_p).wait_recv()
        gather_copy(5, x_g, 1, y_p).start()
        gather_copy(8, x_g, 1, core_p).start()
    with scope('g2'):
        gather_copy(2, y_g, 0, y_p).wait_recv()
        gather_copy(4, y_g, 0, x_p).start()
        gather_copy(10, y_g, 0, core_p).start()
    with scope('g3'):
        core_recv(8, x_g, 1)
        relu_rows(x_g, 1)
        core_recv(10, y_g, 0)
        relu_rows(y_g, 0)
    with scope('g4'):
        gather_copy(1, x_g, 0, x_p).wait_recv()
        gather_copy(9, x_g, 0, core_p).start()
        gather_copy(3, y_g, 1, y_p).wait_recv()
        gather_copy(11, y_g, 1, core_p).start()
    with scope('g5'):
        core_recv(9, x_g, 0)
        relu_rows(x_g, 0)
        core_recv(11, y_g, 1)
        relu_rows(y_g, 1)
    with scope('g6'):
        gather_copy(4, diag_g, 0, x_p).wait_recv()
        gather_copy(12, diag_g, 0, core_p).start()
        gather_copy(5, diag_g, 1, y_p).wait_recv()
        gather_copy(13, diag_g, 1, core_p).start()
    with scope('g7'):
        core_recv(12, diag_g, 0)
        relu_rows(diag_g, 0)
        core_recv(13, diag_g, 1)
        relu_rows(diag_g, 1)

    first_off = low * rows_half
    second_off = rows_half - first_off

    def rows_at(off, n, size):
        return pl.ds(pl.multiple_of(off + n * size, SUB), size)

    def first_rows(u):
        return rows_at(first_off, u, SUB)

    def second_rows(u):
        return rows_at(second_off, u, SUB)

    def slot(u):
        return rows_at(0, u, SUB)

    def first_end(u):
        return remote(y2.at[first_rows(u)], r_first.at[slot(u)], fs_sem.at[0], fr_sem.at[u], inner)

    def first_mid(u):
        return remote(y2.at[first_rows(u)], r_second.at[slot(u)], fs_sem.at[0], sr_sem.at[u], inner)

    def second_mid(u):
        return remote(y2.at[second_rows(u)], r_second.at[slot(u)], ss_sem.at[0], sr_sem.at[u], outer)

    def out_cols(off, v):
        return pl.ds(pl.multiple_of(off + v * OUT_COLS, 128), OUT_COLS)

    def second_out(v):
        return ot.at[:, out_cols(second_off, v)]

    def first_out(v):
        return ot.at[:, out_cols(first_off, v)]

    def out_end(v):
        return remote(second_out(v), second_out(v), us_sem.at[0], ur_sem.at[v], inner)

    def out_far(v, hops):
        dev = {'rows': r, 'rep': lax.rem(z + hops * step + 4, 4)}
        return remote(second_out(v), second_out(v), us_sem.at[0], vr_sem.at[v], dev)

    def out_mid(v):
        return remote(second_out(v), second_out(v), us_sem.at[0], vr_sem.at[v], inner)

    def out_last(v):
        return remote(first_out(v), first_out(v), vs_sem.at[0], vr_sem.at[v], outer)

    def save_second(v):
        return pltpu.make_async_copy(second_out(v), out_hbm.at[:, out_cols(second_off, v)], o_sem.at[0])

    def save_first(v):
        return pltpu.make_async_copy(first_out(v), out_hbm.at[:, out_cols(first_off, v)], o_sem.at[0])

    def event(it, carry):
        t = it - LEAD

        @pl.when(it < 16)
        def _():
            is_second, m = lax.rem(it, 2), it // 2
            off = first_off + is_second * (second_off - first_off)
            rows = rows_at(off, m, mm_rows)
            with scope('mm2'):
                y2[rows, :] = dot(adj[rows, :], zt[...], ((1,), (0,)))

            @pl.when(is_end & (is_second == 0))
            def _():
                for u in range(sub_mm):
                    first_end(m * sub_mm + u).start()

        @pl.when(is_mid & (t >= 0) & (t < n_sub))
        def _():
            with scope('wF'):
                first_end(t).wait_recv()
            y2[first_rows(t), :] = y2[first_rows(t), :] + r_first[slot(t), :]
            first_mid(t).start()

        @pl.when(is_mid & (t >= S_LAG) & (t < n_sub + S_LAG))
        def _():
            u = t - S_LAG
            with scope('wS'):
                first_mid(u).wait_recv()
            y2[second_rows(u), :] = y2[second_rows(u), :] + r_second[slot(u), :]
            second_mid(u).start()

        @pl.when(is_end & (t >= END_LAG) & (t < n_sub + END_LAG) & (lax.rem(t - END_LAG + 64, out_sub) == out_sub - 1))
        def _():
            v = (t - END_LAG) // out_sub
            with scope('wE'):
                for i in range(out_sub):
                    second_mid(v * out_sub + i).wait_recv()
            rows = rows_at(second_off, v, OUT_COLS)
            total = (y2[rows, :] + r_second[rows_at(0, v, OUT_COLS), :]).astype(BF16)
            second_out(v)[...] = dot(w2p[...], total, ((1,), (1,)))[0:f2, :]
            out_end(v).start()

            @pl.when(v >= n_out - DIRECT)
            def _():
                for hops in (2, 3):
                    out_far(v, hops).start()

            save_second(v).start()

        return carry

    lax.fori_loop(0, n_sub + END_LAG + LEAD, event, 0)

    def pass_on(i, carry):
        v = i - OUT_LAG

        @pl.when(is_mid & (i < n_out))
        def _():
            with scope('wOS'):
                out_end(i).wait_recv()

            @pl.when(i < n_out - DIRECT)
            def _():
                out_mid(i).start()

            save_second(i).start()

        @pl.when(is_mid & (i >= OUT_LAG))
        def _():
            with scope('wOF'):
                out_mid(v).wait_recv()

            @pl.when(v < n_out - DIRECT)
            def _():
                out_last(v).start()

            save_first(v).start()

        @pl.when(is_end & (i >= OUT_LAG))
        def _():
            with scope('wOE'):
                out_last(v).wait_recv()
            save_first(v).start()

        return carry

    lax.fori_loop(0, n_out + OUT_LAG, pass_on, 0)

    with scope('drain'):
        def sent(ref, sem):
            remote(ref, ref, sem.at[0], gr_sem.at[0], rows_dev(core_p)).wait_send()

        sent(dbuf, ds_sem)
        sent(xbuf, xs_sem)
        sent(ybuf, ys_sem)
        sent(yt.at[:, 0:14 * piece], gs_sem)
        sent(r_first, fs_sem)
        out_size = n_out * OUT_COLS

        @pl.when(is_end)
        def _():
            sent(ot.at[:, 0:out_size + 2 * DIRECT * OUT_COLS], us_sem)

        @pl.when(is_mid)
        def _():
            sent(r_second, ss_sem)
            sent(ot.at[:, 0:out_size - DIRECT * OUT_COLS], us_sem)
            sent(ot.at[:, 0:out_size - DIRECT * OUT_COLS], vs_sem)

        pltpu.make_async_copy(ot, out_hbm, o_sem.at[0]).wait()


def solution(mesh):
    def local_fn(adj_local, block_mask, feat_blk, w_one, w_two):
        blk, width = adj_local.shape
        f0, f1 = w_one.shape
        f2 = w_two.shape[1]
        f0s = -(-f0 // 8) * 8
        f0p = -(-f0 // 16) * 16
        f2p = -(-f2 // 16) * 16
        piece, rows_half = width // 16, blk // 2
        n_sub, n_out = rows_half // SUB, rows_half // OUT_COLS
        hbm = pl.BlockSpec(memory_space=pl.ANY)
        dma = pltpu.SemaphoreType.DMA
        outt = pl.pallas_call(
            kernel,
            out_shape=jax.ShapeDtypeStruct((f2, blk), F32),
            in_specs=[pl.BlockSpec(memory_space=pltpu.SMEM), hbm, hbm, hbm, hbm],
            out_specs=hbm,
            scratch_shapes=[
                pltpu.VMEM((blk, width), BF16),
                pltpu.VMEM((f0, blk), BF16),
                pltpu.VMEM((f0, f1), BF16),
                pltpu.VMEM((f2, f1), BF16),
                pltpu.VMEM((f0p, blk), BF16),
                pltpu.VMEM((f0p, f1), BF16),
                pltpu.VMEM((f2p, f1), BF16),
                pltpu.VMEM((8, 2, f0s, piece), F32),
                pltpu.VMEM((8, f0s, piece), F32),
                pltpu.VMEM((3, f0s, piece), F32),
                pltpu.VMEM((3, f0s, piece), F32),
                pltpu.VMEM((f0p, width), BF16),
                pltpu.VMEM((width, f1), BF16),
                pltpu.VMEM((blk, f1), F32),
                pltpu.VMEM((rows_half, f1), F32),
                pltpu.VMEM((rows_half, f1), F32),
                pltpu.VMEM((f2, blk), F32),
                dma((8,)), dma((3,)),
                dma((1,)), dma((8,)),
                dma((1,)), dma((3,)), dma((1,)), dma((3,)),
                dma((1,)), dma((14,)),
                dma((1,)), dma((n_sub,)), dma((1,)), dma((n_sub,)),
                dma((1,)), dma((n_out,)), dma((1,)), dma((n_out,)),
                dma((1,)),
            ],
            compiler_params=pltpu.CompilerParams(collective_id=0, has_side_effects=True, vmem_limit_bytes=63 * 1024 * 1024),
        )(block_mask, adj_local, feat_blk.T, w_one, w_two.T)
        return outt.T

    return jax.shard_map(local_fn, mesh=mesh, in_specs=(P('rows', 'rep'), P(), P('rows', None), P(), P()), out_specs=P('rows', None), check_vma=False)
```

```python
import jax
import jax.numpy as jnp
from jax import lax
from jax.experimental import pallas as pl
from jax.experimental.pallas import tpu as pltpu
from jax.sharding import PartitionSpec as P

MESH = pl.DeviceIdType.MESH
BF16 = jnp.bfloat16
F32 = jnp.float32
SUB = 64
OUT_COLS = 128
LEAD = 5
S_LAG = 4
END_LAG = 12
OUT_LAG = 4
EARLY = 2
DIRECT = 2


def dot(a, b, dims):
    return lax.dot_general(a, b, (dims, ((), ())), preferred_element_type=F32)


def scope(name):
    return jax.named_scope(name)


def kernel(mask_hbm, adj_hbm, featt_hbm, w1_hbm, w2t_hbm, out_hbm,
           mask_ref, adj, featt, w1, w2t, ht, w1p, w2p, abuf, dbuf, xbuf, ybuf, yt, zt, y2, r_first, r_second, ot,
           adj_sem, in_sem, ds_sem, dr_sem, xs_sem, xr_sem, ys_sem, yr_sem,
           gs_sem, gr_sem, fs_sem, fr_sem, ss_sem, sr_sem, us_sem, ur_sem, vs_sem, vr_sem, o_sem):
    f0, f2 = featt.shape[0], w2t.shape[0]
    f0s = abuf.shape[2]
    blk, width = adj.shape
    piece = abuf.shape[3]
    block = 2 * piece
    rows_half = blk // 2
    mm_rows = blk // 16
    n_sub = rows_half // SUB
    sub_mm = mm_rows // SUB
    n_out = rows_half // OUT_COLS
    out_sub = OUT_COLS // SUB

    z = lax.axis_index('rep')
    r = lax.axis_index('rows')
    c = lax.rem(r, 2)
    x = lax.rem(r // 2, 2)
    y = r // 4
    core_p = r + 1 - 2 * c
    x_p = r + 2 - 4 * x
    y_p = r + 4 - 8 * y

    low = z // 2
    step = 1 - 2 * low
    inner_z = lax.rem(z + step + 4, 4)
    outer_z = lax.rem(z - step + 4, 4)
    is_end = lax.rem(z, 3) == 0
    is_mid = lax.rem(z, 3) != 0

    def rows_dev(i):
        return {'rows': i, 'rep': z}

    inner, outer = {'rows': r, 'rep': inner_z}, {'rows': r, 'rep': outer_z}

    def group(k):
        ky, kx = lax.rem(k, 2), k // 2
        cy = y * ky + (1 - y) * (1 - ky)
        cx = x * kx + (1 - x) * (1 - kx)
        return 2 * cy + cx

    def block_of(p):
        k = jnp.where(p < 2, 0, jnp.where(p >= 6, 3, jnp.where((p == 2) | (p == 4), 1, 2)))
        h = jnp.where((p == 0) | (p == 2) | (p == 5) | (p == 6), 0, 1)
        return 2 * group(k) + h

    def block_cols(b):
        return pl.ds(pl.multiple_of(b * block, 128), block)

    def adj_copy(p):
        cols = block_cols(block_of(p))
        return pltpu.make_async_copy(adj_hbm.at[:, cols], adj.at[:, cols], adj_sem.at[p])

    in_copies = [pltpu.make_async_copy(src, dst, in_sem.at[i])
                 for i, (src, dst) in enumerate(((featt_hbm, featt), (mask_hbm, mask_ref), (w1_hbm, w1), (w2t_hbm, w2t)))]
    in_copies[0].start()
    in_copies[1].start()
    for p in range(8):
        adj_copy(p).start()
    in_copies[2].start()
    in_copies[3].start()

    barrier = pltpu.get_barrier_semaphore()
    for dev in (core_p, x_p, y_p):
        pl.semaphore_signal(barrier, inc=1, device_id=rows_dev(dev), device_id_type=MESH)
    pl.semaphore_signal(barrier, inc=1, device_id=inner, device_id_type=MESH)

    @pl.when(is_mid)
    def _():
        pl.semaphore_signal(barrier, inc=1, device_id=outer, device_id_type=MESH)

    ht[...] = jnp.zeros_like(ht)
    with scope('feat'):
        in_copies[0].wait()
    ht[0:f0, :] = featt[...]
    with scope('mask'):
        in_copies[1].wait()

    with scope('barrier'):
        pl.semaphore_wait(barrier, jnp.where(is_end, 4, 5))

    def remote(src, dst, send, recv, dev):
        return pltpu.make_async_remote_copy(
            src_ref=src, dst_ref=dst, send_sem=send, recv_sem=recv, device_id=dev, device_id_type=MESH)

    def core_copy(p):
        return remote(abuf.at[p, 1 - c], dbuf.at[p], ds_sem.at[0], dr_sem.at[p], rows_dev(core_p))

    def x_copy(k, p):
        return remote(abuf.at[p, c], xbuf.at[k], xs_sem.at[0], xr_sem.at[k], rows_dev(x_p))

    def y_copy(k, p):
        return remote(abuf.at[p, c], ybuf.at[k], ys_sem.at[0], yr_sem.at[k], rows_dev(y_p))

    def layer_one(p, carry):
        @pl.when(p < 8)
        def _():
            b = block_of(p)
            with scope('adj_wait'):
                adj_copy(p).wait()

            keep = mask_ref[r, 2 * z + b // 4].astype(F32)
            part = dot(ht[...], adj[:, block_cols(b)], ((1,), (0,)))* keep
            abuf[p, 0] = part[:, 0:piece]
            abuf[p, 1] = part[:, piece:block]
            core_copy(p).start()

        @pl.when(p >= 1)
        def _():
            with scope('core_add'):
                core_copy(p - 1).wait_recv()
                abuf[p - 1, c] = abuf[p - 1, c] + dbuf[p - 1]

        @pl.when(p == 1)
        def _():
            x_copy(0, 0).start()

        @pl.when(p == 2)
        def _():
            y_copy(0, 1).start()

        @pl.when(p == 3)
        def _():
            x_copy(1, 2).start()

        @pl.when(p == 4)
        def _():
            y_copy(1, 3).start()

        return carry

    with scope('l1'):
        lax.fori_loop(0, 8, layer_one, 0)

    w1p[...] = jnp.zeros_like(w1p)
    w2p[...] = jnp.zeros_like(w2p)
    in_copies[2].wait()
    w1p[0:f0, :] = w1[...]
    in_copies[3].wait()
    w2p[0:f2, :] = w2t[...]

    with scope('rs0'):
        y_copy(0, 1).wait_recv()
        abuf[4, c] = abuf[4, c] + ybuf[0]
        x_copy(2, 4).start()
    with scope('rs1'):
        x_copy(0, 0).wait_recv()
        abuf[5, c] = abuf[5, c] + xbuf[0]
        y_copy(2, 5).start()
    with scope('rs2'):
        core_copy(7).wait_recv()
        abuf[7, c] = abuf[7, c] + dbuf[7]
    with scope('rs3'):
        y_copy(1, 3).wait_recv()
        abuf[7, c] = abuf[7, c] + ybuf[1]
        x_copy(1, 2).wait_recv()
        abuf[6, c] = abuf[6, c] + xbuf[1]

    own_g, x_g, y_g, diag_g = r // 2, x_p // 2, y_p // 2, y_p // 2 + x_p // 2 - r // 2

    def cols_of(g, h, cc):
        return pl.ds(pl.multiple_of((2 * g + h) * block + cc * piece, 128), piece)

    def gather_copy(k, g, h, dev, cc=None):
        ref = yt.at[:, cols_of(g, h, c if cc is None else cc)]
        return remote(ref, ref, gs_sem.at[0], gr_sem.at[k], rows_dev(dev))

    def core_recv(k, g, h):
        gather_copy(k, g, h, core_p, 1 - c).wait_recv()

    def relu_rows(g, h):
        cols = block_cols(2 * g + h)
        keep = mask_ref[r, 2 * z + g // 2].astype(F32)
        rows = dot(yt[:, cols], w1p[...], ((0,), (0,)))
        zt[cols, :] = (jnp.maximum(rows, 0.0) * keep).astype(BF16)

    with scope('rs4'):
        x_copy(2, 4).wait_recv()
        yt[:, cols_of(own_g, 1, c)] = (abuf[7, c] + xbuf[2]).astype(BF16)
        gather_copy(0, own_g, 1, x_p).start()
        gather_copy(7, own_g, 1, core_p).start()
    with scope('rs5'):
        y_copy(2, 5).wait_recv()
        yt[:, cols_of(own_g, 0, c)] = (abuf[6, c] + ybuf[2]).astype(BF16)
        gather_copy(2, own_g, 0, y_p).start()
        gather_copy(1, own_g, 0, x_p).start()
        gather_copy(3, own_g, 1, y_p).start()
        gather_copy(6, own_g, 0, core_p).start()
    with scope('g0'):
        core_recv(7, own_g, 1)
        relu_rows(own_g, 1)
        core_recv(6, own_g, 0)
        relu_rows(own_g, 0)
    with scope('g1'):
        gather_copy(0, x_g, 1, x_p).wait_recv()
        gather_copy(5, x_g, 1, y_p).start()
        gather_copy(8, x_g, 1, core_p).start()
    with scope('g2'):
        gather_copy(2, y_g, 0, y_p).wait_recv()
        gather_copy(4, y_g, 0, x_p).start()
        gather_copy(10, y_g, 0, core_p).start()
    with scope('g3'):
        core_recv(8, x_g, 1)
        relu_rows(x_g, 1)
        core_recv(10, y_g, 0)
        relu_rows(y_g, 0)
    with scope('g4'):
        gather_copy(1, x_g, 0, x_p).wait_recv()
        gather_copy(9, x_g, 0, core_p).start()
        gather_copy(3, y_g, 1, y_p).wait_recv()
        gather_copy(11, y_g, 1, core_p).start()
    with scope('g5'):
        core_recv(9, x_g, 0)
        relu_rows(x_g, 0)
        core_recv(11, y_g, 1)
        relu_rows(y_g, 1)
    with scope('g6'):
        gather_copy(4, diag_g, 0, x_p).wait_recv()
        gather_copy(12, diag_g, 0, core_p).start()
        gather_copy(5, diag_g, 1, y_p).wait_recv()
        gather_copy(13, diag_g, 1, core_p).start()
    with scope('g7'):
        core_recv(12, diag_g, 0)
        relu_rows(diag_g, 0)
        core_recv(13, diag_g, 1)
        relu_rows(diag_g, 1)

    first_off = low * rows_half
    second_off = rows_half - first_off

    def rows_at(off, n, size):
        return pl.ds(pl.multiple_of(off + n * size, SUB), size)

    def first_rows(u):
        return rows_at(first_off, u, SUB)

    def second_rows(u):
        return rows_at(second_off, u, SUB)

    def slot(u):
        return rows_at(0, u, SUB)

    def first_end(u):
        return remote(y2.at[first_rows(u)], r_first.at[slot(u)], fs_sem.at[0], fr_sem.at[u], inner)

    def first_mid(u):
        return remote(y2.at[first_rows(u)], r_second.at[slot(u)], fs_sem.at[0], sr_sem.at[u], inner)

    def second_mid(u):
        return remote(y2.at[second_rows(u)], r_second.at[slot(u)], ss_sem.at[0], sr_sem.at[u], outer)

    def out_cols(off, v):
        return pl.ds(pl.multiple_of(off + v * OUT_COLS, 128), OUT_COLS)

    def second_out(v):
        return ot.at[:, out_cols(second_off, v)]

    def first_out(v):
        return ot.at[:, out_cols(first_off, v)]

    def out_end(v):
        return remote(second_out(v), second_out(v), us_sem.at[0], ur_sem.at[v], inner)

    def out_far(v, hops):
        dev = {'rows': r, 'rep': lax.rem(z + hops * step + 4, 4)}
        return remote(second_out(v), second_out(v), us_sem.at[0], vr_sem.at[v], dev)

    def out_mid(v):
        return remote(second_out(v), second_out(v), us_sem.at[0], vr_sem.at[v], inner)

    def out_last(v):
        return remote(first_out(v), first_out(v), vs_sem.at[0], vr_sem.at[v], outer)

    def save_second(v):
        return pltpu.make_async_copy(second_out(v), out_hbm.at[:, out_cols(second_off, v)], o_sem.at[0])

    def save_first(v):
        return pltpu.make_async_copy(first_out(v), out_hbm.at[:, out_cols(first_off, v)], o_sem.at[0])

    def pass_on(i):
        v = i - OUT_LAG

        @pl.when(i < n_out)
        def _():
            with scope('wOS'):
                out_end(i).wait_recv()

            @pl.when(i < n_out - DIRECT)
            def _():
                out_mid(i).start()

            save_second(i).start()

        @pl.when((i >= OUT_LAG))
        def _():
            with scope('wOF'):
                out_mid(v).wait_recv()

            @pl.when(v < n_out - DIRECT)
            def _():
                out_last(v).start()

            save_first(v).start()

    def event(it, carry):
        t = it - LEAD

        @pl.when(it < 16)
        def _():
            is_second, m = lax.rem(it, 2), it // 2
            off = first_off + is_second * (second_off - first_off)
            rows = rows_at(off, m, mm_rows)
            with scope('mm2'):
                y2[rows, :] = dot(adj[rows, :], zt[...], ((1,), (0,)))

            @pl.when(is_end & (is_second == 0))
            def _():
                for u in range(sub_mm):
                    first_end(m * sub_mm + u).start()

        @pl.when(is_mid & (t >= 0) & (t < n_sub))
        def _():
            with scope('wF'):
                first_end(t).wait_recv()
            y2[first_rows(t), :] = y2[first_rows(t), :] + r_first[slot(t), :]
            first_mid(t).start()

        @pl.when(is_mid & (t >= S_LAG) & (t < n_sub + S_LAG))
        def _():
            u = t - S_LAG
            with scope('wS'):
                first_mid(u).wait_recv()
            y2[second_rows(u), :] = y2[second_rows(u), :] + r_second[slot(u), :]
            second_mid(u).start()

        @pl.when(is_end & (t >= END_LAG) & (t < n_sub + END_LAG) & (lax.rem(t - END_LAG + 64, out_sub) == out_sub - 1))
        def _():
            v = (t - END_LAG) // out_sub
            with scope('wE'):
                for i in range(out_sub):
                    second_mid(v * out_sub + i).wait_recv()
            rows = rows_at(second_off, v, OUT_COLS)
            total = (y2[rows, :] + r_second[rows_at(0, v, OUT_COLS), :]).astype(BF16)
            second_out(v)[...] = dot(w2p[...], total, ((1,), (1,)))[0:f2, :]
            out_end(v).start()

            @pl.when(v >= n_out - DIRECT)
            def _():
                for hops in (2, 3):
                    out_far(v, hops).start()

            save_second(v).start()

        @pl.when(is_mid & (t >= n_sub) & (t < n_sub + S_LAG))
        def _():
            for i in range(EARLY):
                pass_on((t - n_sub) * EARLY + i)

        return carry

    lax.fori_loop(0, n_sub + END_LAG + LEAD, event, 0)

    def rest(i, carry):
        pl.when(is_mid & (i >= S_LAG * EARLY))(lambda: pass_on(i))

        @pl.when(is_end & (i >= OUT_LAG))
        def _():
            with scope('wOE'):
                out_last(i - OUT_LAG).wait_recv()
            save_first(i - OUT_LAG).start()

        return carry

    lax.fori_loop(0, n_out + OUT_LAG, rest, 0)


    with scope('drain'):
        def sent(ref, sem):
            remote(ref, ref, sem.at[0], gr_sem.at[0], rows_dev(core_p)).wait_send()

        sent(dbuf, ds_sem)
        sent(xbuf, xs_sem)
        sent(ybuf, ys_sem)
        sent(yt.at[:, 0:14 * piece], gs_sem)
        sent(r_first, fs_sem)
        out_size = n_out * OUT_COLS

        @pl.when(is_end)
        def _():
            sent(ot.at[:, 0:out_size + 2 * DIRECT * OUT_COLS], us_sem)

        @pl.when(is_mid)
        def _():
            sent(r_second, ss_sem)
            sent(ot.at[:, 0:out_size - DIRECT * OUT_COLS], us_sem)
            sent(ot.at[:, 0:out_size - DIRECT * OUT_COLS], vs_sem)

        pltpu.make_async_copy(ot, out_hbm, o_sem.at[0]).wait()


def solution(mesh):
    def local_fn(adj_local, block_mask, feat_blk, w_one, w_two):
        blk, width = adj_local.shape
        f0, f1 = w_one.shape
        f2 = w_two.shape[1]
        f0s = -(-f0 // 8) * 8
        f2p = -(-f2 // 16) * 16
        piece, rows_half = width // 16, blk // 2
        n_sub, n_out = rows_half // SUB, rows_half // OUT_COLS
        hbm = pl.BlockSpec(memory_space=pl.ANY)
        dma = pltpu.SemaphoreType.DMA
        outt = pl.pallas_call(
            kernel,
            out_shape=jax.ShapeDtypeStruct((f2, blk), F32),
            in_specs=[hbm] * 5,
            out_specs=hbm,
            scratch_shapes=[
                pltpu.SMEM(block_mask.shape, block_mask.dtype),
                pltpu.VMEM((blk, width), BF16),
                pltpu.VMEM((f0, blk), BF16),
                pltpu.VMEM((f0, f1), BF16),
                pltpu.VMEM((f2, f1), BF16),
                pltpu.VMEM((f0s, blk), BF16),
                pltpu.VMEM((f0s, f1), BF16),
                pltpu.VMEM((f2p, f1), BF16),
                pltpu.VMEM((8, 2, f0s, piece), F32),
                pltpu.VMEM((8, f0s, piece), F32),
                pltpu.VMEM((3, f0s, piece), F32),
                pltpu.VMEM((3, f0s, piece), F32),
                pltpu.VMEM((f0s, width), BF16),
                pltpu.VMEM((width, f1), BF16),
                pltpu.VMEM((blk, f1), F32),
                pltpu.VMEM((rows_half, f1), F32),
                pltpu.VMEM((rows_half, f1), F32),
                pltpu.VMEM((f2, blk), F32),
                dma((8,)), dma((4,)),
                dma((1,)), dma((8,)),
                dma((1,)), dma((3,)), dma((1,)), dma((3,)),
                dma((1,)), dma((14,)),
                dma((1,)), dma((n_sub,)), dma((1,)), dma((n_sub,)),
                dma((1,)), dma((n_out,)), dma((1,)), dma((n_out,)),
                dma((1,)),
            ],
            compiler_params=pltpu.CompilerParams(collective_id=0, has_side_effects=True, vmem_limit_bytes=63 * 1024 * 1024),
        )(block_mask, adj_local, feat_blk.T, w_one, w_two.T)
        return outt.T

    return jax.shard_map(local_fn, mesh=mesh, in_specs=(P('rows', 'rep'), P(), P('rows', None), P(), P()), out_specs=P('rows', None), check_vma=False)
```

```python
import jax
import jax.numpy as jnp
from jax import lax
from jax.experimental import pallas as pl
from jax.experimental.pallas import tpu as pltpu
from jax.sharding import PartitionSpec as P

MESH = pl.DeviceIdType.MESH
BF16 = jnp.bfloat16
F32 = jnp.float32
SUB = 32
OUT_COLS = 128
LEAD = 4
S_LAGS = (7, 3)
END_LAG = 24
OUT_LAG = 4
DIRECT = 2


def dot(a, b, dims):
    return lax.dot_general(a, b, (dims, ((), ())), preferred_element_type=F32)


def scope(name):
    return jax.named_scope(name)


def kernel(mask_hbm, adj_hbm, featt_hbm, w1_hbm, w2t_hbm, out_hbm,
           mask_ref, adj, featt, w1, w2t, ht, w1p, w2p, abuf, dbuf, xbuf, ybuf, yt, zt, y2, r_first, r_second, ot,
           adj_sem, in_sem, ds_sem, dr_sem, xs_sem, xr_sem, ys_sem, yr_sem,
           gs_sem, gr_sem, fs_sem, fr_sem, ss_sem, sr_sem, us_sem, ur_sem, vs_sem, vr_sem, o_sem):
    f0, f2 = featt.shape[0], w2t.shape[0]
    f0s = abuf.shape[2]
    blk, width = adj.shape
    piece = abuf.shape[3]
    block = 2 * piece
    rows_half = blk // 2
    mm_rows = blk // 16
    n_sub = rows_half // SUB
    sub_mm = mm_rows // SUB
    n_out = rows_half // OUT_COLS
    out_sub = OUT_COLS // SUB

    z = lax.axis_index('rep')
    r = lax.axis_index('rows')
    c = lax.rem(r, 2)
    x = lax.rem(r // 2, 2)
    y = r // 4
    core_p = r + 1 - 2 * c
    x_p = r + 2 - 4 * x
    y_p = r + 4 - 8 * y

    low = z // 2
    step = 1 - 2 * low
    inner_z = lax.rem(z + step + 4, 4)
    outer_z = lax.rem(z - step + 4, 4)
    is_end = lax.rem(z, 3) == 0
    is_mid = lax.rem(z, 3) != 0

    def rows_dev(i):
        return {'rows': i, 'rep': z}

    inner, outer = {'rows': r, 'rep': inner_z}, {'rows': r, 'rep': outer_z}

    def group(k):
        ky, kx = lax.rem(k, 2), k // 2
        cy = y * ky + (1 - y) * (1 - ky)
        cx = x * kx + (1 - x) * (1 - kx)
        return 2 * cy + cx

    def block_of(p):
        k = jnp.where(p < 2, 0, jnp.where(p >= 6, 3, jnp.where((p == 2) | (p == 4), 1, 2)))
        h = jnp.where((p == 0) | (p == 2) | (p == 5) | (p == 6), 0, 1)
        return 2 * group(k) + h

    def block_cols(b):
        return pl.ds(pl.multiple_of(b * block, 128), block)

    def adj_copy(p):
        cols = block_cols(block_of(p))
        return pltpu.make_async_copy(adj_hbm.at[:, cols], adj.at[:, cols], adj_sem.at[p])

    in_copies = [pltpu.make_async_copy(src, dst, in_sem.at[i])
                 for i, (src, dst) in enumerate(((featt_hbm, featt), (mask_hbm, mask_ref), (w1_hbm, w1), (w2t_hbm, w2t)))]
    in_copies[0].start()
    in_copies[1].start()
    for p in range(8):
        adj_copy(p).start()
    in_copies[2].start()
    in_copies[3].start()

    barrier = pltpu.get_barrier_semaphore()
    for dev in (core_p, x_p, y_p):
        pl.semaphore_signal(barrier, inc=1, device_id=rows_dev(dev), device_id_type=MESH)
    pl.semaphore_signal(barrier, inc=1, device_id=inner, device_id_type=MESH)

    @pl.when(is_mid)
    def _():
        pl.semaphore_signal(barrier, inc=1, device_id=outer, device_id_type=MESH)

    ht[...] = jnp.zeros_like(ht)
    with scope('feat'):
        in_copies[0].wait()
    ht[0:f0, :] = featt[...]
    with scope('mask'):
        in_copies[1].wait()

    with scope('barrier'):
        pl.semaphore_wait(barrier, jnp.where(is_end, 4, 5))

    def remote(src, dst, send, recv, dev):
        return pltpu.make_async_remote_copy(
            src_ref=src, dst_ref=dst, send_sem=send, recv_sem=recv, device_id=dev, device_id_type=MESH)

    def core_copy(p):
        return remote(abuf.at[p, 1 - c], dbuf.at[p], ds_sem.at[0], dr_sem.at[p], rows_dev(core_p))

    def x_copy(k, p):
        return remote(abuf.at[p, c], xbuf.at[k], xs_sem.at[0], xr_sem.at[k], rows_dev(x_p))

    def y_copy(k, p):
        return remote(abuf.at[p, c], ybuf.at[k], ys_sem.at[0], yr_sem.at[k], rows_dev(y_p))

    def layer_one(p, carry):
        @pl.when(p == 7)
        def _():
            with scope('rs0'):
                y_copy(0, 1).wait_recv()
                abuf[4, c] = abuf[4, c] + ybuf[0]
                x_copy(2, 4).start()
            with scope('rs1'):
                x_copy(0, 0).wait_recv()
                abuf[5, c] = abuf[5, c] + xbuf[0]
                y_copy(2, 5).start()

        @pl.when(p < 8)
        def _():
            b = block_of(p)
            with scope('adj_wait'):
                adj_copy(p).wait()

            keep = mask_ref[r, 2 * z + b // 4].astype(F32)
            part = dot(ht[...], adj[:, block_cols(b)], ((1,), (0,)))* keep
            abuf[p, 0] = part[:, 0:piece]
            abuf[p, 1] = part[:, piece:block]
            core_copy(p).start()

        @pl.when(p >= 1)
        def _():
            with scope('core_add'):
                core_copy(p - 1).wait_recv()
                abuf[p - 1, c] = abuf[p - 1, c] + dbuf[p - 1]

        @pl.when(p == 1)
        def _():
            x_copy(0, 0).start()

        @pl.when(p == 2)
        def _():
            y_copy(0, 1).start()

        @pl.when(p == 3)
        def _():
            x_copy(1, 2).start()

        @pl.when(p == 4)
        def _():
            y_copy(1, 3).start()

        return carry

    with scope('l1'):
        lax.fori_loop(0, 8, layer_one, 0)

    w1p[...] = jnp.zeros_like(w1p)
    w2p[...] = jnp.zeros_like(w2p)
    in_copies[2].wait()
    w1p[0:f0, :] = w1[...]
    in_copies[3].wait()
    w2p[0:f2, :] = w2t[...]

    with scope('rs2'):
        core_copy(7).wait_recv()
        abuf[7, c] = abuf[7, c] + dbuf[7]
    with scope('rs3'):
        y_copy(1, 3).wait_recv()
        abuf[7, c] = abuf[7, c] + ybuf[1]
        x_copy(1, 2).wait_recv()
        abuf[6, c] = abuf[6, c] + xbuf[1]

    own_g, x_g, y_g, diag_g = r // 2, x_p // 2, y_p // 2, y_p // 2 + x_p // 2 - r // 2

    def cols_of(g, h, cc):
        return pl.ds(pl.multiple_of((2 * g + h) * block + cc * piece, 128), piece)

    def gather_copy(k, g, h, dev, cc=None):
        ref = yt.at[:, cols_of(g, h, c if cc is None else cc)]
        return remote(ref, ref, gs_sem.at[0], gr_sem.at[k], rows_dev(dev))

    def core_recv(k, g, h):
        gather_copy(k, g, h, core_p, 1 - c).wait_recv()

    def relu_rows(g, h):
        cols = block_cols(2 * g + h)
        keep = mask_ref[r, 2 * z + g // 2].astype(F32)
        rows = dot(yt[:, cols], w1p[...], ((0,), (0,)))
        zt[cols, :] = (jnp.maximum(rows, 0.0) * keep).astype(BF16)

    first_off = low * rows_half
    second_off = rows_half - first_off
    s_lag = jnp.where(low == 0, S_LAGS[0], S_LAGS[1])

    def rows_at(off, n, size):
        return pl.ds(pl.multiple_of(off + n * size, SUB), size)

    head = rows_at(first_off, 0, mm_rows)

    def add_head(g, h):
        cols = block_cols(2 * g + h)
        y2[head, :] += dot(adj[head, cols], zt[cols, :], ((1,), (0,)))

    with scope('rs4'):
        x_copy(2, 4).wait_recv()
        yt[:, cols_of(own_g, 1, c)] = (abuf[7, c] + xbuf[2]).astype(BF16)
        gather_copy(0, own_g, 1, x_p).start()
        gather_copy(7, own_g, 1, core_p).start()
    with scope('rs5'):
        y_copy(2, 5).wait_recv()
        yt[:, cols_of(own_g, 0, c)] = (abuf[6, c] + ybuf[2]).astype(BF16)
        gather_copy(2, own_g, 0, y_p).start()
        gather_copy(1, own_g, 0, x_p).start()
        gather_copy(3, own_g, 1, y_p).start()
        gather_copy(6, own_g, 0, core_p).start()
    with scope('g0'):
        core_recv(7, own_g, 1)
        relu_rows(own_g, 1)
        core_recv(6, own_g, 0)
        relu_rows(own_g, 0)
        y2[head, :] = jnp.zeros((mm_rows, y2.shape[1]), F32)
        add_head(own_g, 0)
        add_head(own_g, 1)
    with scope('g1'):
        gather_copy(0, x_g, 1, x_p).wait_recv()
        gather_copy(5, x_g, 1, y_p).start()
        gather_copy(8, x_g, 1, core_p).start()
    with scope('g2'):
        gather_copy(2, y_g, 0, y_p).wait_recv()
        gather_copy(4, y_g, 0, x_p).start()
        gather_copy(10, y_g, 0, core_p).start()
    with scope('g3'):
        core_recv(8, x_g, 1)
        relu_rows(x_g, 1)
        core_recv(10, y_g, 0)
        relu_rows(y_g, 0)
        add_head(x_g, 1)
        add_head(y_g, 0)
    with scope('g4'):
        gather_copy(1, x_g, 0, x_p).wait_recv()
        gather_copy(9, x_g, 0, core_p).start()
        gather_copy(3, y_g, 1, y_p).wait_recv()
        gather_copy(11, y_g, 1, core_p).start()
    with scope('g5'):
        core_recv(9, x_g, 0)
        relu_rows(x_g, 0)
        core_recv(11, y_g, 1)
        relu_rows(y_g, 1)
    with scope('g6'):
        gather_copy(4, diag_g, 0, x_p).wait_recv()
        gather_copy(12, diag_g, 0, core_p).start()
        gather_copy(5, diag_g, 1, y_p).wait_recv()
        gather_copy(13, diag_g, 1, core_p).start()
    with scope('g7'):
        core_recv(12, diag_g, 0)
        relu_rows(diag_g, 0)
        core_recv(13, diag_g, 1)
        relu_rows(diag_g, 1)

    def first_rows(u):
        return rows_at(first_off, u, SUB)

    def second_rows(u):
        return rows_at(second_off, u, SUB)

    def slot(u):
        return rows_at(0, u, SUB)

    def first_end(u):
        return remote(y2.at[first_rows(u)], r_first.at[slot(u)], fs_sem.at[0], fr_sem.at[u], inner)

    def first_mid(u):
        return remote(y2.at[first_rows(u)], r_second.at[slot(u)], fs_sem.at[0], sr_sem.at[u], inner)

    def second_mid(u):
        return remote(y2.at[second_rows(u)], r_second.at[slot(u)], ss_sem.at[0], sr_sem.at[u], outer)

    def out_cols(off, v):
        return pl.ds(pl.multiple_of(off + v * OUT_COLS, 128), OUT_COLS)

    def second_out(v):
        return ot.at[:, out_cols(second_off, v)]

    def first_out(v):
        return ot.at[:, out_cols(first_off, v)]

    def out_end(v):
        return remote(second_out(v), second_out(v), us_sem.at[0], ur_sem.at[v], inner)

    def out_far(v, hops):
        dev = {'rows': r, 'rep': lax.rem(z + hops * step + 4, 4)}
        return remote(second_out(v), second_out(v), us_sem.at[0], vr_sem.at[v], dev)

    def out_mid(v):
        return remote(second_out(v), second_out(v), us_sem.at[0], vr_sem.at[v], inner)

    def out_last(v):
        return remote(first_out(v), first_out(v), vs_sem.at[0], vr_sem.at[v], outer)

    def save_second(v):
        return pltpu.make_async_copy(second_out(v), out_hbm.at[:, out_cols(second_off, v)], o_sem.at[0])

    def save_first(v):
        return pltpu.make_async_copy(first_out(v), out_hbm.at[:, out_cols(first_off, v)], o_sem.at[0])

    n_fwd = n_out - DIRECT

    def near(i):
        with scope('wOS'):
            out_end(i).wait_recv()

        @pl.when(i < n_fwd)
        def _():
            out_mid(i).start()

        save_second(i).start()

    def far(v):
        with scope('wOF'):
            out_last(v).wait_recv()

        @pl.when(is_mid & (v < n_fwd))
        def _():
            out_last(v).start()

        save_first(v).start()

    def send_first(m):
        @pl.when(is_end)
        def _():
            for u in range(sub_mm):
                first_end(m * sub_mm + u).start()

    with scope('head'):
        add_head(x_g, 0)
        add_head(y_g, 1)
        add_head(diag_g, 0)
        add_head(diag_g, 1)
    send_first(0)

    def event(it, carry):
        t = it - LEAD

        @pl.when((it < LEAD) | ((lax.rem(it - LEAD, 2) == 0) & (t < 2 * (16 - LEAD))))
        def _():
            i = jnp.where(it < LEAD, it, LEAD + t // 2)
            is_second, m = lax.rem(i, 2), i // 2
            off = first_off + is_second * (second_off - first_off)
            rows = rows_at(off, m, mm_rows)
            with scope('mm2'):
                y2[rows, :] = dot(adj[rows, :], zt[...], ((1,), (0,)))
            pl.when(is_second == 0)(lambda: send_first(m))

        @pl.when(is_mid & (t >= 0) & (t < n_sub))
        def _():
            with scope('wF'):
                first_end(t).wait_recv()
            y2[first_rows(t), :] = y2[first_rows(t), :] + r_first[slot(t), :]
            first_mid(t).start()

        @pl.when(is_mid & (t >= s_lag) & (t < n_sub + s_lag))
        def _():
            u = t - s_lag
            with scope('wS'):
                first_mid(u).wait_recv()
            y2[second_rows(u), :] = y2[second_rows(u), :] + r_second[slot(u), :]
            second_mid(u).start()

        @pl.when(is_mid & (t >= n_sub) & (t < n_sub + s_lag))
        def _():
            near(t - n_sub)

        @pl.when(is_end & (t >= END_LAG) & (lax.rem(t - END_LAG + 64, out_sub) == out_sub - 1))
        def _():
            v = (t - END_LAG) // out_sub
            with scope('wE'):
                for i in range(out_sub):
                    second_mid(v * out_sub + i).wait_recv()
            rows = rows_at(second_off, v, OUT_COLS)
            total = (y2[rows, :] + r_second[rows_at(0, v, OUT_COLS), :]).astype(BF16)
            second_out(v)[...] = dot(w2p[...], total, ((1,), (1,)))[0:f2, :]
            out_end(v).start()

            @pl.when(v >= n_fwd)
            def _():
                for hops in (2, 3):
                    out_far(v, hops).start()

            save_second(v).start()

        return carry

    lax.fori_loop(1, n_sub + END_LAG + LEAD, event, 0)

    def pass_on(i, carry):
        pl.when(is_mid & (i >= s_lag) & (i < n_fwd))(lambda: near(i))
        pl.when(i >= OUT_LAG)(lambda: far(i - OUT_LAG))
        return carry

    lax.fori_loop(0, n_fwd + OUT_LAG, pass_on, 0)

    for v in range(n_fwd, n_out):
        pl.when(is_mid)(lambda: near(v))
        far(v)

    with scope('drain'):
        def sent(ref, sem):
            remote(ref, ref, sem.at[0], gr_sem.at[0], rows_dev(core_p)).wait_send()

        sent(dbuf, ds_sem)
        sent(xbuf, xs_sem)
        sent(ybuf, ys_sem)
        sent(yt.at[:, 0:14 * piece], gs_sem)
        sent(r_first, fs_sem)
        out_size = n_out * OUT_COLS

        @pl.when(is_end)
        def _():
            sent(ot.at[:, 0:out_size + 2 * DIRECT * OUT_COLS], us_sem)

        @pl.when(is_mid)
        def _():
            sent(r_second, ss_sem)
            sent(ot.at[:, 0:out_size - DIRECT * OUT_COLS], us_sem)
            sent(ot.at[:, 0:out_size - DIRECT * OUT_COLS], vs_sem)

        pltpu.make_async_copy(ot, out_hbm, o_sem.at[0]).wait()


def solution(mesh):
    def local_fn(adj_local, block_mask, feat_blk, w_one, w_two):
        blk, width = adj_local.shape
        f0, f1 = w_one.shape
        f2 = w_two.shape[1]
        f0s = -(-f0 // 8) * 8
        f2p = -(-f2 // 16) * 16
        piece, rows_half = width // 16, blk // 2
        n_sub, n_out = rows_half // SUB, rows_half // OUT_COLS
        hbm = pl.BlockSpec(memory_space=pl.ANY)
        dma = pltpu.SemaphoreType.DMA
        outt = pl.pallas_call(
            kernel,
            out_shape=jax.ShapeDtypeStruct((f2, blk), F32),
            in_specs=[hbm] * 5,
            out_specs=hbm,
            scratch_shapes=[
                pltpu.SMEM(block_mask.shape, block_mask.dtype),
                pltpu.VMEM((blk, width), BF16),
                pltpu.VMEM((f0, blk), BF16),
                pltpu.VMEM((f0, f1), BF16),
                pltpu.VMEM((f2, f1), BF16),
                pltpu.VMEM((f0s, blk), BF16),
                pltpu.VMEM((f0s, f1), BF16),
                pltpu.VMEM((f2p, f1), BF16),
                pltpu.VMEM((8, 2, f0s, piece), F32),
                pltpu.VMEM((8, f0s, piece), F32),
                pltpu.VMEM((3, f0s, piece), F32),
                pltpu.VMEM((3, f0s, piece), F32),
                pltpu.VMEM((f0s, width), BF16),
                pltpu.VMEM((width, f1), BF16),
                pltpu.VMEM((blk, f1), F32),
                pltpu.VMEM((rows_half, f1), F32),
                pltpu.VMEM((rows_half, f1), F32),
                pltpu.VMEM((f2, blk), F32),
                dma((8,)), dma((4,)),
                dma((1,)), dma((8,)),
                dma((1,)), dma((3,)), dma((1,)), dma((3,)),
                dma((1,)), dma((14,)),
                dma((1,)), dma((n_sub,)), dma((1,)), dma((n_sub,)),
                dma((1,)), dma((n_out,)), dma((1,)), dma((n_out,)),
                dma((1,)),
            ],
            compiler_params=pltpu.CompilerParams(collective_id=0, has_side_effects=True, vmem_limit_bytes=63 * 1024 * 1024),
        )(block_mask, adj_local, feat_blk.T, w_one, w_two.T)
        return outt.T

    return jax.shard_map(local_fn, mesh=mesh, in_specs=(P('rows', 'rep'), P(), P('rows', None), P(), P()), out_specs=P('rows', None), check_vma=False)
```

```python
import jax
import jax.numpy as jnp
from jax import lax
from jax.experimental import pallas as pl
from jax.experimental.pallas import tpu as pltpu
from jax.sharding import PartitionSpec as P

MESH = pl.DeviceIdType.MESH
BF16 = jnp.bfloat16
F32 = jnp.float32
SUB = 32
OUT_COLS = 128
PARTS = 3
LEAD = 3
S_LAGS = (7, 2)
END_LAG = 24
DIRECT = 4


def dot(a, b, dims):
    return lax.dot_general(a, b, (dims, ((), ())), preferred_element_type=F32)


def scope(name):
    return jax.named_scope(name)


def kernel(mask_hbm, adj_hbm, featt_hbm, w1_hbm, w2t_hbm, out_ref,
           mask_ref, adj, featt, w1, w2t, ht, w1p, w2p, abuf, dbuf, xbuf, ybuf, yt, zt, y2, r_first, r_second, ot,
           adj_sem, in_sem, ds_sem, dr_sem, xs_sem, xr_sem, ys_sem, yr_sem,
           gs_sem, gr_sem, hr_sem, fs_sem, fr_sem, ss_sem, sr_sem, us_sem, ur_sem, vs_sem, vr_sem):
    f0, f2 = featt.shape[0], w2t.shape[0]
    f0s = abuf.shape[2]
    blk, width = adj.shape
    piece = abuf.shape[3]
    block = 2 * piece
    rows_half = blk // 2
    mm_rows = blk // 16
    n_sub = rows_half // SUB
    sub_mm = mm_rows // SUB
    n_out = rows_half // OUT_COLS
    out_sub = OUT_COLS // SUB

    z = lax.axis_index('rep')
    r = lax.axis_index('rows')
    c = lax.rem(r, 2)
    x = lax.rem(r // 2, 2)
    y = r // 4
    core_p = r + 1 - 2 * c
    x_p = r + 2 - 4 * x
    y_p = r + 4 - 8 * y

    low = z // 2
    step = 1 - 2 * low
    inner_z = lax.rem(z + step + 4, 4)
    outer_z = lax.rem(z - step + 4, 4)
    is_end = lax.rem(z, 3) == 0
    is_mid = lax.rem(z, 3) != 0

    def rows_dev(i):
        return {'rows': i, 'rep': z}

    inner, outer = {'rows': r, 'rep': inner_z}, {'rows': r, 'rep': outer_z}

    def group(k):
        ky, kx = lax.rem(k, 2), k // 2
        cy = y * ky + (1 - y) * (1 - ky)
        cx = x * kx + (1 - x) * (1 - kx)
        return 2 * cy + cx

    def block_of(p):
        k = jnp.where(p < 2, 0, jnp.where(p >= 6, 3, jnp.where((p == 2) | (p == 4), 1, 2)))
        h = jnp.where((p == 0) | (p == 2) | (p == 5) | (p == 6), 0, 1)
        return 2 * group(k) + h

    def block_cols(b):
        return pl.ds(pl.multiple_of(b * block, 128), block)

    def adj_copy(p):
        cols = block_cols(block_of(p))
        return pltpu.make_async_copy(adj_hbm.at[:, cols], adj.at[:, cols], adj_sem.at[p])

    in_copies = [pltpu.make_async_copy(src, dst, in_sem.at[i])
                 for i, (src, dst) in enumerate(((featt_hbm, featt), (mask_hbm, mask_ref), (w1_hbm, w1), (w2t_hbm, w2t)))]
    in_copies[0].start()
    in_copies[1].start()
    for p in range(8):
        adj_copy(p).start()
    in_copies[2].start()
    in_copies[3].start()

    barrier = pltpu.get_barrier_semaphore()
    for dev in (core_p, x_p, y_p):
        pl.semaphore_signal(barrier, inc=1, device_id=rows_dev(dev), device_id_type=MESH)
    pl.semaphore_signal(barrier, inc=1, device_id=inner, device_id_type=MESH)

    @pl.when(is_mid)
    def _():
        pl.semaphore_signal(barrier, inc=1, device_id=outer, device_id_type=MESH)

    ht[...] = jnp.zeros_like(ht)
    with scope('feat'):
        in_copies[0].wait()
    ht[0:f0, :] = featt[...]
    with scope('mask'):
        in_copies[1].wait()

    with scope('barrier'):
        pl.semaphore_wait(barrier, jnp.where(is_end, 4, 5))

    def remote(src, dst, send, recv, dev):
        return pltpu.make_async_remote_copy(
            src_ref=src, dst_ref=dst, send_sem=send, recv_sem=recv, device_id=dev, device_id_type=MESH)

    def core_copy(p):
        return remote(abuf.at[p, 1 - c], dbuf.at[p], ds_sem.at[0], dr_sem.at[p], rows_dev(core_p))

    def x_copy(k, p):
        return remote(abuf.at[p, c], xbuf.at[k], xs_sem.at[0], xr_sem.at[k], rows_dev(x_p))

    def y_copy(k, p):
        return remote(abuf.at[p, c], ybuf.at[k], ys_sem.at[0], yr_sem.at[k], rows_dev(y_p))

    def layer_one(p, carry):
        @pl.when(p == 7)
        def _():
            with scope('rs0'):
                y_copy(0, 1).wait_recv()
                abuf[4, c] = abuf[4, c] + ybuf[0]
                x_copy(2, 4).start()
            with scope('rs1'):
                x_copy(0, 0).wait_recv()
                abuf[5, c] = abuf[5, c] + xbuf[0]
                y_copy(2, 5).start()

        @pl.when(p < 8)
        def _():
            b = block_of(p)
            with scope('adj_wait'):
                adj_copy(p).wait()

            keep = mask_ref[r, 2 * z + b // 4].astype(F32)
            part = dot(ht[...], adj[:, block_cols(b)], ((1,), (0,)))* keep
            abuf[p, 0] = part[:, 0:piece]
            abuf[p, 1] = part[:, piece:block]
            core_copy(p).start()

        @pl.when(p >= 1)
        def _():
            with scope('core_add'):
                core_copy(p - 1).wait_recv()
                abuf[p - 1, c] = abuf[p - 1, c] + dbuf[p - 1]

        @pl.when(p == 1)
        def _():
            x_copy(0, 0).start()

        @pl.when(p == 2)
        def _():
            y_copy(0, 1).start()

        @pl.when(p == 3)
        def _():
            x_copy(1, 2).start()

        @pl.when(p == 4)
        def _():
            y_copy(1, 3).start()

        return carry

    with scope('l1'):
        lax.fori_loop(0, 8, layer_one, 0)

    w1p[...] = jnp.zeros_like(w1p)
    w2p[...] = jnp.zeros_like(w2p)
    in_copies[2].wait()
    w1p[0:f0, :] = w1[...]
    in_copies[3].wait()
    w2p[0:f2, :] = w2t[...]

    with scope('rs2'):
        core_copy(7).wait_recv()
        abuf[7, c] = abuf[7, c] + dbuf[7]
    with scope('rs3'):
        y_copy(1, 3).wait_recv()
        abuf[7, c] = abuf[7, c] + ybuf[1]
        x_copy(1, 2).wait_recv()
        abuf[6, c] = abuf[6, c] + xbuf[1]

    own_g, x_g, y_g, diag_g = r // 2, x_p // 2, y_p // 2, y_p // 2 + x_p // 2 - r // 2

    def cols_of(g, h, cc):
        return pl.ds(pl.multiple_of((2 * g + h) * block + cc * piece, 128), piece)

    def gather_copy(k, g, h, dev, cc=None):
        ref = yt.at[:, cols_of(g, h, c if cc is None else cc)]
        return remote(ref, ref, gs_sem.at[0], gr_sem.at[k], rows_dev(dev))

    def part_copy(k, i, g, h, dev):
        size = piece // PARTS
        ref = yt.at[:, pl.ds(pl.multiple_of((2 * g + h) * block + c * piece + i * size, 128), size)]
        return remote(ref, ref, gs_sem.at[0], hr_sem.at[k, i], rows_dev(dev))

    def part_send(k, g, h, dev):
        for i in range(PARTS):
            part_copy(k, i, g, h, dev).start()

    def part_pass(k, g, h, dev, k_out, dev_out):
        for i in range(PARTS):
            part_copy(k, i, g, h, dev).wait_recv()
            part_copy(k_out, i, g, h, dev_out).start()

    def part_recv(k, g, h, dev):
        for i in range(PARTS):
            part_copy(k, i, g, h, dev).wait_recv()

    def core_recv(k, g, h):
        gather_copy(k, g, h, core_p, 1 - c).wait_recv()

    def relu_rows(g, h):
        cols = block_cols(2 * g + h)
        keep = mask_ref[r, 2 * z + g // 2].astype(F32)
        rows = dot(yt[:, cols], w1p[...], ((0,), (0,)))
        zt[cols, :] = (jnp.maximum(rows, 0.0) * keep).astype(BF16)

    first_off = low * rows_half
    second_off = rows_half - first_off
    s_lag = jnp.where(low == 0, S_LAGS[0], S_LAGS[1])

    def rows_at(off, n, size):
        return pl.ds(pl.multiple_of(off + n * size, SUB), size)

    head = rows_at(first_off, 0, mm_rows)

    def group_sum(g):
        cols = pl.ds(pl.multiple_of(g * 2 * block, 128), 2 * block)
        return dot(adj[head, cols], zt[cols, :], ((1,), (0,)))

    with scope('rs4'):
        x_copy(2, 4).wait_recv()
        yt[:, cols_of(own_g, 1, c)] = (abuf[7, c] + xbuf[2]).astype(BF16)
        part_send(0, own_g, 1, x_p)
        gather_copy(7, own_g, 1, core_p).start()
    with scope('rs5'):
        y_copy(2, 5).wait_recv()
        yt[:, cols_of(own_g, 0, c)] = (abuf[6, c] + ybuf[2]).astype(BF16)
        part_send(1, own_g, 0, y_p)
        gather_copy(1, own_g, 0, x_p).start()
        gather_copy(3, own_g, 1, y_p).start()
        gather_copy(6, own_g, 0, core_p).start()
    with scope('g0'):
        core_recv(7, own_g, 1)
        relu_rows(own_g, 1)
        core_recv(6, own_g, 0)
        relu_rows(own_g, 0)
        y2[head, :] = group_sum(own_g)
    with scope('g1'):
        part_pass(0, x_g, 1, x_p, 3, y_p)
        gather_copy(8, x_g, 1, core_p).start()
    with scope('g2'):
        part_pass(1, y_g, 0, y_p, 2, x_p)
        gather_copy(10, y_g, 0, core_p).start()
    with scope('g3'):
        core_recv(8, x_g, 1)
        relu_rows(x_g, 1)
        core_recv(10, y_g, 0)
        relu_rows(y_g, 0)
    with scope('g4'):
        gather_copy(1, x_g, 0, x_p).wait_recv()
        gather_copy(9, x_g, 0, core_p).start()
        gather_copy(3, y_g, 1, y_p).wait_recv()
        gather_copy(11, y_g, 1, core_p).start()
    with scope('g5'):
        core_recv(9, x_g, 0)
        relu_rows(x_g, 0)
        core_recv(11, y_g, 1)
        relu_rows(y_g, 1)
    with scope('g6'):
        part_recv(2, diag_g, 0, x_p)
        gather_copy(12, diag_g, 0, core_p).start()
        y2[head, :] += group_sum(x_g)
        part_recv(3, diag_g, 1, y_p)
        gather_copy(13, diag_g, 1, core_p).start()
        y2[head, :] += group_sum(y_g)
    with scope('g7'):
        core_recv(12, diag_g, 0)
        relu_rows(diag_g, 0)
        core_recv(13, diag_g, 1)
        relu_rows(diag_g, 1)

    def first_rows(u):
        return rows_at(first_off, u, SUB)

    def second_rows(u):
        return rows_at(second_off, u, SUB)

    def slot(u):
        return rows_at(0, u, SUB)

    def first_end(u):
        return remote(y2.at[first_rows(u)], r_first.at[slot(u)], fs_sem.at[0], fr_sem.at[u], inner)

    def first_mid(u):
        return remote(y2.at[first_rows(u)], r_second.at[slot(u)], fs_sem.at[0], sr_sem.at[u], inner)

    def second_mid(u):
        return remote(y2.at[second_rows(u)], r_second.at[slot(u)], ss_sem.at[0], sr_sem.at[u], outer)

    def out_cols(off, v):
        return pl.ds(pl.multiple_of(off + v * OUT_COLS, 128), OUT_COLS)

    def second_out(v):
        return ot.at[:, out_cols(second_off, v)]

    def first_out(v):
        return ot.at[:, out_cols(first_off, v)]

    def out_end(v):
        return remote(second_out(v), second_out(v), us_sem.at[0], ur_sem.at[v], inner)

    def out_far(v, hops):
        dev = {'rows': r, 'rep': lax.rem(z + hops * step + 4, 4)}
        return remote(second_out(v), second_out(v), us_sem.at[0], vr_sem.at[v], dev)

    def out_mid(v):
        return remote(second_out(v), second_out(v), us_sem.at[0], vr_sem.at[v], inner)

    def out_last(v):
        return remote(first_out(v), first_out(v), vs_sem.at[0], vr_sem.at[v], outer)

    n_fwd = n_out - DIRECT

    def near(i):
        with scope('wOS'):
            out_end(i).wait_recv()

        @pl.when(i < n_fwd)
        def _():
            out_mid(i).start()

    def far(v):
        with scope('wOF'):
            out_last(v).wait_recv()

        @pl.when(is_mid & (v < n_fwd))
        def _():
            out_last(v).start()

    def send_first(m):
        @pl.when(is_end)
        def _():
            for u in range(sub_mm):
                first_end(m * sub_mm + u).start()

    with scope('head'):
        y2[head, :] += group_sum(diag_g)
    send_first(0)

    def event(it, carry):
        t = it - LEAD

        @pl.when((it < LEAD) | ((lax.rem(it - LEAD, 2) == 0) & (t < 2 * (16 - LEAD))))
        def _():
            i = jnp.where(it < LEAD, it, LEAD + t // 2)
            is_second, m = lax.rem(i, 2), i // 2
            off = first_off + is_second * (second_off - first_off)
            rows = rows_at(off, m, mm_rows)
            with scope('mm2'):
                y2[rows, :] = dot(adj[rows, :], zt[...], ((1,), (0,)))
            pl.when(is_second == 0)(lambda: send_first(m))

        @pl.when(is_mid & (t >= 0) & (t < n_sub))
        def _():
            with scope('wF'):
                first_end(t).wait_recv()
            y2[first_rows(t), :] = y2[first_rows(t), :] + r_first[slot(t), :]
            first_mid(t).start()

        @pl.when(is_mid & (t >= s_lag) & (t < n_sub + s_lag))
        def _():
            u = t - s_lag
            with scope('wS'):
                first_mid(u).wait_recv()
            y2[second_rows(u), :] = y2[second_rows(u), :] + r_second[slot(u), :]
            second_mid(u).start()

        @pl.when(is_mid & (t >= n_sub) & (t < n_sub + s_lag))
        def _():
            near(t - n_sub)

        @pl.when(is_end & (t >= END_LAG) & (lax.rem(t - END_LAG + 64, out_sub) == out_sub - 1))
        def _():
            v = (t - END_LAG) // out_sub
            with scope('wE'):
                for i in range(out_sub):
                    second_mid(v * out_sub + i).wait_recv()
            rows = rows_at(second_off, v, OUT_COLS)
            total = (y2[rows, :] + r_second[rows_at(0, v, OUT_COLS), :]).astype(BF16)
            second_out(v)[...] = dot(w2p[...], total, ((1,), (1,)))[0:f2, :]

            @pl.when(v >= n_fwd)
            def _():
                for hops in (3, 2):
                    out_far(v, hops).start()

            out_end(v).start()

        return carry

    lax.fori_loop(1, LEAD + n_sub + jnp.where(is_end, END_LAG, s_lag), event, 0)

    @pl.when(is_mid)
    def _():
        def forward(i, carry):
            near(i)
            return carry

        lax.fori_loop(s_lag, n_fwd, forward, 0)

    def arrive(v, carry):
        far(v)
        return carry

    lax.fori_loop(0, n_out, arrive, 0)

    @pl.when(is_mid)
    def _():
        def last(v, carry):
            near(v)
            return carry

        lax.fori_loop(n_fwd, n_out, last, 0)

    with scope('drain'):
        def sent(ref, sem):
            remote(ref, ref, sem.at[0], gr_sem.at[0], rows_dev(core_p)).wait_send()

        sent(dbuf, ds_sem)
        sent(xbuf, xs_sem)
        sent(ybuf, ys_sem)
        sent(yt.at[:, 0:14 * piece], gs_sem)
        sent(r_first, fs_sem)
        out_size = n_out * OUT_COLS

        @pl.when(is_end)
        def _():
            sent(ot.at[:, 0:out_size + 2 * DIRECT * OUT_COLS], us_sem)

        @pl.when(is_mid)
        def _():
            sent(r_second, ss_sem)
            sent(ot.at[:, 0:out_size - DIRECT * OUT_COLS], us_sem)
            sent(ot.at[:, 0:out_size - DIRECT * OUT_COLS], vs_sem)

    out_ref[...] = ot[...]


def solution(mesh):
    def local_fn(adj_local, block_mask, feat_blk, w_one, w_two):
        blk, width = adj_local.shape
        f0, f1 = w_one.shape
        f2 = w_two.shape[1]
        f0s = -(-f0 // 8) * 8
        f2p = -(-f2 // 16) * 16
        piece, rows_half = width // 16, blk // 2
        n_sub, n_out = rows_half // SUB, rows_half // OUT_COLS
        hbm = pl.BlockSpec(memory_space=pltpu.HBM)
        dma = pltpu.SemaphoreType.DMA
        outt = pl.pallas_call(
            kernel,
            out_shape=pltpu.VMEM((f2, blk), F32),
            in_specs=[hbm] * 5,
            out_specs=pl.BlockSpec(memory_space=pltpu.VMEM),
            scratch_shapes=[
                pltpu.SMEM(block_mask.shape, block_mask.dtype),
                pltpu.VMEM((blk, width), BF16),
                pltpu.VMEM((f0, blk), BF16),
                pltpu.VMEM((f0, f1), BF16),
                pltpu.VMEM((f2, f1), BF16),
                pltpu.VMEM((f0s, blk), BF16),
                pltpu.VMEM((f0s, f1), BF16),
                pltpu.VMEM((f2p, f1), BF16),
                pltpu.VMEM((8, 2, f0s, piece), F32),
                pltpu.VMEM((8, f0s, piece), F32),
                pltpu.VMEM((3, f0s, piece), F32),
                pltpu.VMEM((3, f0s, piece), F32),
                pltpu.VMEM((f0s, width), BF16),
                pltpu.VMEM((width, f1), BF16),
                pltpu.VMEM((blk, f1), F32),
                pltpu.VMEM((rows_half, f1), F32),
                pltpu.VMEM((rows_half, f1), F32),
                pltpu.VMEM((f2, blk), F32),
                dma((8,)), dma((4,)),
                dma((1,)), dma((8,)),
                dma((1,)), dma((3,)), dma((1,)), dma((3,)),
                dma((1,)), dma((14,)), dma((4, PARTS)),
                dma((1,)), dma((n_sub,)), dma((1,)), dma((n_sub,)),
                dma((1,)), dma((n_out,)), dma((1,)), dma((n_out,)),
            ],
            compiler_params=pltpu.CompilerParams(collective_id=0, has_side_effects=True, vmem_limit_bytes=60 * 1024 * 1024),
        )(block_mask, adj_local, feat_blk.T, w_one, w_two.T)
        return outt.T

    return jax.shard_map(local_fn, mesh=mesh, in_specs=(P('rows', 'rep'), P(), P('rows', None), P(), P()), out_specs=P('rows', None), check_vma=False)
```
